32 devices in a mesh: dp: 4 (over y, x), fsdp: 8 (over z, core).
Axes of the slice: x: 2, y: 2, z: 4, core: 2. Of those that a mesh axis runs over, the one named last changes fastest.
Arguments:
- tokens: bfloat16 [512, 3072], P('dp'), may hold values from -6 to 6
- cotangent: bfloat16 [512, 3072], P('dp'), may hold values from -6 to 6
- routes: int32 [512, 2], P('dp'), may hold values from 0 to 3, all different within a row; in each aligned block of 128 rows (0 to 127, 128 to 255, ...) at most 64 rows name the same one
- router_weight: float32 [512, 2], P('dp'), may hold values from 0.25 to 1
- w_gate: bfloat16 [4, 3072, 8192], P('dp', None, 'fsdp'), may hold values from -0.109375 to 0.109375
- w_up: bfloat16 [4, 3072, 8192], P('dp', None, 'fsdp'), may hold values from -0.109375 to 0.109375
- w_down: bfloat16 [4, 8192, 3072], P('dp', 'fsdp'), may hold values from -0.0625 to 0.0625
Outputs:
- output: bfloat16 [512, 3072], P('dp')
- input_grad: bfloat16 [512, 3072], P('dp')
- grad_gate: bfloat16 [4, 3072, 8192], P('dp', None, 'fsdp')
- grad_up: bfloat16 [4, 3072, 8192], P('dp', None, 'fsdp')
- grad_down: bfloat16 [4, 8192, 3072], P('dp', 'fsdp')
The draws below stay inside these ranges and needn't reach their ends.
Inputs may be any that keep to these rules, and one draw needn't show every extreme that they name: `routes`: the two experts of a token differ. In the 128 rows of one batch no expert is named by more than 64 rows, a bound that some block reaches in some batches.
All inputs are finite; a program needn't handle non-finite values.
Results may differ from the reference program's by a relative error of at most 0.025.
Values may be sent and summed in bfloat16 or wider, within the bound.
A program may use at most 128 MiB of HBM per device.

```python
import math
import jax
import jax.numpy as jnp
import numpy as np
from jax import lax

D = 3072
F = 8192
TOK_DEV = 128
EXPERTS = 4
CAP = 64
TOKENS = 512
N_DP = 4
N_FSDP = 8


def levels(rng, shape, shards, low, top_value):
    level = 1.0
    for dim, parts in shards:
        heights = jax.random.uniform(jax.random.fold_in(jax.random.fold_in(rng, 6), dim), (parts,), jnp.float32, low / len(shards), top_value / len(shards))
        level = level * jnp.repeat(jnp.exp(heights), shape[dim] // parts).reshape((-1,) + (1,) * (len(shape) - 1 - dim))
    return level


def assign_block(stream_key, own, number, rows, count, top, limit, lean):
    sequence = jax.random.permutation(stream_key, count)
    crowded, common = portions_of(count, rows * top, limit, lean, True), portions_of(count, rows * top, limit, lean, False)
    places = jnp.arange(count)

    def named(lengths, offset_by):
        used = int((lengths > 0).sum())
        fixed = max(1, used // 4)
        passed = fixed + (places - fixed + offset_by * (used - fixed)) % max(1, count - fixed)
        return jnp.zeros((count,), jnp.int32).at[sequence[jnp.where(places < fixed, places, passed)]].set(jnp.asarray(lengths, jnp.int32))

    lengths = jnp.where(number % 4 == 0, named(crowded, number // 4), named(common, number - number // 4 - 1))
    mixed = jax.random.permutation(jax.random.fold_in(own, 3), count)
    source_of, sink = mixed[0:count // 2 * 2:2], mixed[1:count // 2 * 2:2]
    room = jnp.minimum(lengths[source_of] - 1, limit - lengths[sink]) // 2
    room = jnp.where((source_of == sequence[0]) | (sink == sequence[0]) | (lengths[sink] == 0), 0, jnp.maximum(room, 0))
    passed = jax.random.randint(jax.random.fold_in(own, 4), (count // 2,), 0, 1 << 20) % (room + 1)
    lengths = lengths.at[source_of].add(-passed).at[sink].add(passed)
    labels = jnp.searchsorted(jnp.cumsum(lengths), jnp.arange(rows * top), side="right").astype(jnp.int32)
    grid = labels.reshape(top, rows).T
    grid = grid[jax.random.permutation(jax.random.fold_in(own, 1), rows)]
    offset_by = jax.random.randint(jax.random.fold_in(own, 2), (rows, 1), 0, top)
    return jnp.take_along_axis(grid, (jnp.arange(top)[None, :] + offset_by) % top, axis=1)


def portions_of(number_of, total, bound, skew, full):
    portions = [(1 << 20) // math.isqrt(grade ** skew) + 1 for grade in range(1, number_of + 1)]
    largest = bound if full else min(bound, max(-(-total // number_of), total * portions[0] // sum(portions)))
    least = 1 if total - largest >= number_of - 1 else 0
    given, surplus = [largest] + [least] * (number_of - 1), total - largest - least * (number_of - 1)
    while surplus > 0:
        candidates = [i for i in range(1, number_of) if given[i] < largest] or [i for i in range(1, number_of) if given[i] < bound]
        whole, budget = sum([portions[i] for i in candidates]), surplus
        for i in candidates:
            extra = min(bound - given[i], max(1, budget * portions[i] // whole), surplus)
            given[i] = given[i] + extra
            surplus = surplus - extra
    return np.array(given)


def bell_draw(key, extent, width, bound, split=(), kind=jnp.bfloat16):
    gain = levels(key, extent, split, -0.22, 0.18) if split else 1.0
    entries = jax.random.normal(key, extent, jnp.float32) * width * gain
    return jnp.minimum(jnp.maximum(entries, -bound), bound).astype(kind)


def setup_inputs(seed: int = 0) -> dict:
    seeds = jax.random.split(jax.random.key(seed), 8)
    tokens = bell_draw(seeds[0], (TOKENS, D), 1.0, 6.0, ((0, 4),))
    cotangent = bell_draw(seeds[1], (TOKENS, D), 1.0, 6.0, ((0, 4),))
    routes_keys = jax.random.split(jax.random.fold_in(seeds[2], 1), TOKENS // TOK_DEV)
    routes_turns = jax.random.permutation(jax.random.fold_in(seeds[2], 3), TOKENS // TOK_DEV)
    routes = jax.vmap(lambda own, number: assign_block(jax.random.fold_in(seeds[2], 2), own, number, TOK_DEV, N_DP, 2, CAP, 1))(routes_keys, routes_turns).reshape((TOKENS, 2))
    router_weight = jnp.clip(0.25 + 0.75 * jax.random.uniform(seeds[3], (TOKENS, 2), jnp.float32) ** levels(seeds[3], (TOKENS, 2), ((0, 4),), -0.2, 0.2), 0.25, 1.0)
    w_gate = bell_draw(seeds[4], (EXPERTS, D, F), D ** -0.5, 0.109375, ((0, 4), (2, 8)))
    w_up = bell_draw(seeds[5], (EXPERTS, D, F), D ** -0.5, 0.109375, ((0, 4), (2, 8)))
    w_down = bell_draw(seeds[6], (EXPERTS, F, D), F ** -0.5, 0.0625, ((0, 4), (1, 8)))
    return dict(tokens=tokens, cotangent=cotangent, routes=routes, router_weight=router_weight, w_gate=w_gate, w_up=w_up, w_down=w_down)


def slot_tables(routes, router_weight):
    expert_ids = jnp.arange(N_DP, dtype=jnp.int32)
    hit_table = (routes[..., None] == expert_ids).astype(jnp.int32)
    per_token = jnp.sum(hit_table, axis=2)
    before = jnp.cumsum(per_token, axis=1) - per_token
    slot_of = jnp.sum(hit_table * before[:, :, None, :], axis=3)
    slot_ids = jnp.arange(CAP, dtype=jnp.int32)
    placed = hit_table[..., None] * (slot_of[..., None, None] == slot_ids).astype(jnp.int32)
    picked = jnp.sum(placed, axis=2).astype(jnp.float32)
    weighted = jnp.sum(placed.astype(jnp.float32) * router_weight[..., None, None], axis=2)
    return picked, weighted


def expert_pass(operands):
    slot_x, slot_dy, gate_w, up_w, down_w = operands
    gate_pre = jnp.dot(slot_x, gate_w, preferred_element_type=jnp.float32)
    up_pre = jnp.dot(slot_x, up_w, preferred_element_type=jnp.float32)
    sigma = jax.nn.sigmoid(gate_pre)
    active = gate_pre * sigma
    hidden = (active * up_pre).astype(jnp.bfloat16)
    hidden_dy = jnp.dot(slot_dy, down_w.T, preferred_element_type=jnp.float32)
    gate_dy = (hidden_dy * up_pre * sigma * (1.0 + gate_pre * (1.0 - sigma))).astype(jnp.bfloat16)
    up_dy = (hidden_dy * active).astype(jnp.bfloat16)
    grad_down = jnp.dot(hidden.T, slot_dy, preferred_element_type=jnp.float32).astype(jnp.bfloat16)
    grad_gate = jnp.dot(slot_x.T, gate_dy, preferred_element_type=jnp.float32).astype(jnp.bfloat16)
    grad_up = jnp.dot(slot_x.T, up_dy, preferred_element_type=jnp.float32).astype(jnp.bfloat16)
    block_width = F // N_FSDP

    def one_block(carry, index):
        start = (index * block_width).astype(jnp.int32)
        hidden_part = lax.dynamic_slice_in_dim(hidden, start, block_width, 1)
        gate_part = lax.dynamic_slice_in_dim(gate_dy, start, block_width, 1)
        up_part = lax.dynamic_slice_in_dim(up_dy, start, block_width, 1)
        down_rows = lax.dynamic_slice_in_dim(down_w, start, block_width, 0)
        gate_cols = lax.dynamic_slice_in_dim(gate_w, start, block_width, 1)
        up_cols = lax.dynamic_slice_in_dim(up_w, start, block_width, 1)
        out_term = jnp.dot(hidden_part, down_rows, preferred_element_type=jnp.float32).astype(jnp.bfloat16)
        out_term = lax.optimization_barrier(out_term)
        back_term = (jnp.dot(gate_part, gate_cols.T, preferred_element_type=jnp.float32)
                     + jnp.dot(up_part, up_cols.T, preferred_element_type=jnp.float32)).astype(jnp.bfloat16)
        back_term = lax.optimization_barrier(back_term)
        return (carry[0] + out_term.astype(jnp.float32), carry[1] + back_term.astype(jnp.float32)), None

    zeros = jnp.zeros((slot_x.shape[0], D), jnp.float32)
    totals, unused = lax.scan(one_block, (zeros, zeros), jnp.arange(N_FSDP, dtype=jnp.int32))
    return totals[0].astype(jnp.bfloat16), totals[1].astype(jnp.bfloat16), grad_gate, grad_up, grad_down


def reference(tokens, cotangent, routes, router_weight, w_gate, w_up, w_down):
    blocks = TOKENS // TOK_DEV
    highest = lax.Precision.HIGHEST
    inputs = tokens.reshape(blocks, TOK_DEV, D).astype(jnp.float32)
    grads_in = cotangent.reshape(blocks, TOK_DEV, D).astype(jnp.float32)
    picked, weighted = slot_tables(routes.reshape(blocks, TOK_DEV, 2), router_weight.reshape(blocks, TOK_DEV, 2))
    slot_x = jnp.einsum('btec,btd->ebcd', picked, inputs, precision=highest).astype(jnp.bfloat16)
    slot_dy = jnp.einsum('btec,btd->ebcd', weighted, grads_in, precision=highest).astype(jnp.bfloat16)
    slot_x = slot_x.reshape(N_DP, blocks * CAP, D)
    slot_dy = slot_dy.reshape(N_DP, blocks * CAP, D)
    slot_out, slot_dx, grad_gate, grad_up, grad_down = lax.map(expert_pass, (slot_x, slot_dy, w_gate, w_up, w_down))
    slot_out = slot_out.reshape(N_DP, blocks, CAP, D).astype(jnp.float32)
    slot_dx = slot_dx.reshape(N_DP, blocks, CAP, D).astype(jnp.float32)
    output = jnp.einsum('btec,ebcd->btd', weighted, slot_out, precision=highest).astype(jnp.bfloat16)
    input_grad = jnp.einsum('btec,ebcd->btd', picked, slot_dx, precision=highest).astype(jnp.bfloat16)
    return (output.reshape(TOKENS, D), input_grad.reshape(TOKENS, D), grad_gate, grad_up, grad_down)
```

```python
import functools

import jax
import jax.numpy as jnp
from jax import lax
from jax.experimental import pallas as pl
from jax.experimental.pallas import tpu as pltpu
from jax.sharding import PartitionSpec as P

MESH = pl.DeviceIdType.MESH
BF16 = jnp.bfloat16
F32 = jnp.float32
LEAD = (((0,), (0,)), ((), ()))
TRAIL = (((1,), (1,)), ((), ()))


def flip(a, mask):
    bit = 1
    while bit <= mask:
        if mask & bit:
            a = a + bit - 2 * bit * ((a // bit) % 2)
        bit *= 2
    return a


def xor(v, a, n):
    out = v - v
    bit = 1
    while bit < n:
        x, y = (v // bit) % 2, (a // bit) % 2
        out = out + bit * (x + y - 2 * x * y)
        bit *= 2
    return out


def mm(a, b, dims=(((1,), (0,)), ((), ()))):
    return lax.dot_general(a, b, dims, preferred_element_type=F32)


def routed_kernel(
    n, cap, tile, wide, width,
    tokens_hbm, cotangent_hbm, routes_hbm, rweight_hbm, wg_hbm, wu_hbm, wd_hbm,
    output, input_grad, x_turned, dy_rows, hid_turned, hid_dy,
    tok, cot, rts, rwt, wg, wu, wd, slots, snd, gpre, upre, hid,
    core_snd, core_rcv, own, ret_snd, ret, part, from_outer, joint, from_inner, fin,
    w_sem, a_send, a_recv, d_send, d_recv, f_send, f_recv, c_send, c_recv, r_send, r_recv,
    s_send, s_recv, j_send, j_recv, g_send, g_recv, h_send, h_recv,
):
    d = lax.axis_index("dp")
    f = lax.axis_index("fsdp")
    c = f % 2
    z = f // 2
    sib = (d, flip(f, 1))
    pair = (d, flip(f, 2))
    across = (d, 2 * (3 - z) + c)
    outer = (z % 3) == 0
    inner = (z % 3) != 0
    toks, features = tok.shape
    half = features // 2
    rows = n * cap
    units = gpre.shape[1]
    chunks = half // width
    order = sorted(range(1, n), key=lambda m: -bin(m).count("1"))
    far = order[0]
    near = order[1:]
    share = cap // 2

    def remote(src, dst, ssem, rsem, dev):
        return pltpu.make_async_remote_copy(
            src_ref=src, dst_ref=dst, send_sem=ssem, recv_sem=rsem,
            device_id=dev, device_id_type=MESH,
        )

    barrier = pltpu.get_barrier_semaphore()
    friends = [(flip(d, m), f) for m in order] + [sib, pair, across]
    for dev in friends:
        pl.semaphore_signal(barrier, inc=1, device_id=dev, device_id_type=MESH)

    loads = [
        pltpu.make_async_copy(s, t, w_sem.at[k])
        for k, (s, t) in enumerate(
            (
                (routes_hbm, rts), (rweight_hbm, rwt), (tokens_hbm, tok), (cotangent_hbm, cot),
                (wg_hbm, wg), (wu_hbm, wu), (wd_hbm, wd),
            )
        )
    ]
    for load in loads:
        load.start()
    loads[0].wait()
    loads[1].wait()

    slot_row = lax.broadcasted_iota(jnp.int32, (rows, toks), 0)
    m_of = slot_row // cap
    e_of = xor(m_of, d, n)
    s_of = (slot_row % cap).astype(F32)
    r = rts[...]
    hit0 = r[0:1, :] == e_of
    hit1 = r[1:2, :] == e_of
    per_token = jnp.where(hit0 | hit1, 1.0, 0.0).astype(BF16)
    earlier = (
        lax.broadcasted_iota(jnp.int32, (toks, toks), 0)
        < lax.broadcasted_iota(jnp.int32, (toks, toks), 1)
    )
    before = mm(per_token, jnp.where(earlier, 1.0, 0.0).astype(BF16))
    here = before == s_of
    first = jnp.where(hit0 & here, 1.0, 0.0)
    second = jnp.where(hit1 & here, 1.0, 0.0)
    rw = rwt[...]
    slot_weight = jnp.sum(first * rw[0:1, :] + second * rw[1:2, :], axis=1, keepdims=True)
    picked = (first + second).astype(BF16)
    same = (
        lax.broadcasted_iota(jnp.int32, (toks, toks), 0)
        == lax.broadcasted_iota(jnp.int32, (toks, toks), 1)
    )
    back = mm(jnp.where(same, 1.0, 0.0).astype(BF16), picked, TRAIL).astype(BF16)

    mine = pl.ds(pl.multiple_of(c * half, 128), half)
    other = pl.ds(pl.multiple_of((1 - c) * half, 128), half)

    def build(t):
        src = (tok, cot)[t]
        v = mm(picked, src[:, mine])
        u = mm(picked[:cap], src[:, other])
        if t:
            v = v * slot_weight
            u = u * slot_weight[:cap]
        snd[t] = v.astype(BF16).reshape(n, cap, half)
        slots[c, t, 0] = v[:cap].astype(BF16)
        slots[1 - c, t, 0] = u.astype(BF16)

    held = pl.ds(pl.multiple_of((z % 2) * share, 16), share)
    missing = pl.ds(pl.multiple_of((1 - z % 2) * share, 16), share)
    sends = []

    def start(cp):
        cp.start()
        sends.append((None, cp))

    def direct(t, m):
        dev = (flip(d, m), f)
        if m == far:
            return remote(
                snd.at[t, m, held], slots.at[c, t, m, held], a_send.at[t, m], a_recv.at[t, m], dev
            )
        return remote(snd.at[t, m], slots.at[c, t, m], a_send.at[t, m], a_recv.at[t, m], dev)

    def dispatch(t):
        for m in order:
            start(direct(t, m))

    def relay(t, rows_at):
        piece = slots.at[c, t, far, rows_at]
        return remote(piece, piece, d_send.at[t], d_recv.at[t], pair)

    def forward(t, k, h):
        if k == 0:
            piece = slots.at[h, t, far, held]
        elif k == n:
            piece = slots.at[h, t, far, missing]
        else:
            piece = slots.at[h, t, k]
        return remote(piece, piece, f_send.at[t, k], f_recv.at[t, k], sib)

    def relay_far(t):
        direct(t, far).wait_recv()
        start(relay(t, held))
        start(forward(t, 0, c))

    def collect(t):
        for m in near:
            direct(t, m).wait_recv()
            start(forward(t, m, c))
        relay(t, missing).wait_recv()
        start(forward(t, n, c))

    def collected(t):
        for k in [0] + near + [n]:
            forward(t, k, 1 - c).wait_recv()

    loads[2].wait()
    build(0)
    pl.semaphore_wait(barrier, len(friends))
    dispatch(0)
    loads[3].wait()
    build(1)
    dispatch(1)

    def at_half(h):
        return pl.ds(pl.multiple_of(h * half, 128), half)

    def activate(at, cols, g, u):
        gpre[at, cols] = g
        upre[at, cols] = u
        hid[at, cols] = (g * jax.nn.sigmoid(g) * u).astype(BF16)

    self_rows = pl.ds(0, cap)
    their_rows = pl.ds(cap, rows - cap)

    def self_gate(j, carry):
        cols = pl.ds(pl.multiple_of(j * tile, tile), tile)
        gpre[self_rows, cols] = mm(slots[0, 0, 0], wg[pl.ds(0, half), cols]) + mm(
            slots[1, 0, 0], wg[pl.ds(half, half), cols]
        )
        return carry

    def self_up(j, carry):
        cols = pl.ds(pl.multiple_of(j * tile, tile), tile)
        u = mm(slots[0, 0, 0], wu[pl.ds(0, half), cols]) + mm(
            slots[1, 0, 0], wu[pl.ds(half, half), cols]
        )
        activate(self_rows, cols, gpre[self_rows, cols], u)
        return carry

    def near_half(j, carry):
        cols = pl.ds(pl.multiple_of(j * tile, tile), tile)
        x = slots[c, 0, 1:].reshape(rows - cap, half)
        gpre[their_rows, cols] = mm(x, wg[at_half(c), cols])
        upre[their_rows, cols] = mm(x, wu[at_half(c), cols])
        return carry

    def far_half(j, carry):
        cols = pl.ds(pl.multiple_of(j * tile, tile), tile)
        x = slots[1 - c, 0, 1:].reshape(rows - cap, half)
        g = gpre[their_rows, cols] + mm(x, wg[at_half(1 - c), cols])
        u = upre[their_rows, cols] + mm(x, wu[at_half(1 - c), cols])
        activate(their_rows, cols, g, u)
        return carry

    loads[4].wait()
    with jax.named_scope("self_gate"):
        lax.fori_loop(0, units // tile, self_gate, 0)
    with jax.named_scope("relay0"):
        relay_far(0)
    loads[5].wait()
    with jax.named_scope("self_up"):
        lax.fori_loop(0, units // tile, self_up, 0)
    with jax.named_scope("collect0"):
        collect(0)
    with jax.named_scope("near_half"):
        lax.fori_loop(0, units // tile, near_half, 0)
    with jax.named_scope("collected0"):
        collected(0)
    with jax.named_scope("far_half"):
        lax.fori_loop(0, units // tile, far_half, 0)
    loads[6].wait()
    with jax.named_scope("relay1"):
        relay_far(1)

    def swap(t, q):
        return remote(core_snd.at[t, q], core_rcv.at[t, q], c_send.at[t, q], c_recv.at[t, q], sib)

    def returned(t, q, m):
        return remote(
            ret_snd.at[t, q, m], ret.at[t, q, m], r_send.at[t, q, m], r_recv.at[t, q, m],
            (flip(d, m), f),
        )

    per = wide // width

    def project(t, term, between):
        def theirs(k):
            at = pl.multiple_of((1 - c) * half + k * wide, 128)
            v = term(pl.ds(at, wide)).astype(BF16)
            for i in range(per):
                q = k * per + i
                core_snd[t, q] = v[:, i * width : (i + 1) * width].reshape(n, cap, width)
                start(swap(t, q))

        def ours(k):
            at = pl.multiple_of(c * half + k * wide, 128)
            own[t, k] = term(pl.ds(at, wide))

        def finish(k):
            for i in range(per):
                q = k * per + i
                swap(t, q).wait_recv()
                for m in order + [0]:
                    v = own[t, k, m * cap : (m + 1) * cap, i * width : (i + 1) * width]
                    v = (v + core_rcv[t, q, m].astype(F32)).astype(BF16)
                    if m:
                        ret_snd[t, q, m] = v
                        start(returned(t, q, m))
                    else:
                        ret[t, q, 0] = v

        count = half // wide
        theirs(0)
        ours(0)
        for k in range(1, count):
            theirs(k)
            finish(k - 1)
            ours(k)
        between()
        finish(count - 1)

    with jax.named_scope("project0"):
        project(0, lambda cols: mm(hid[...], wd[:, cols]), lambda: None)
    with jax.named_scope("collect1"):
        collect(1)
        collected(1)

    def down_step(j, carry):
        cols = pl.ds(pl.multiple_of(j * tile, tile), tile)
        hdy = mm(slots[0, 1].reshape(rows, half), wd[cols, pl.ds(0, half)], TRAIL) + mm(
            slots[1, 1].reshape(rows, half), wd[cols, pl.ds(half, half)], TRAIL
        )
        g = gpre[:, cols]
        sig = jax.nn.sigmoid(g)
        hid_dy[0, :, cols] = (hdy * upre[:, cols] * sig * (1.0 + g * (1.0 - sig))).astype(BF16)
        hid_dy[1, :, cols] = (hdy * (g * sig)).astype(BF16)
        return carry

    with jax.named_scope("down"):
        lax.fori_loop(0, units // tile, down_step, 0)
    with jax.named_scope("project1"):
        project(
            1,
            lambda cols: mm(hid_dy[0], wg[cols, :], TRAIL) + mm(hid_dy[1], wu[cols, :], TRAIL),
            lambda: None,
        )

    def outward(t, q):
        return remote(
            part.at[t, q], from_outer.at[t, q], s_send.at[t, q], s_recv.at[t, q], pair
        )

    def middle(t, q):
        return remote(
            joint.at[t, q], from_inner.at[t, q], j_send.at[t, q], j_recv.at[t, q], across
        )

    def spread(t, q):
        piece = fin.at[c, t, q]
        return remote(piece, piece, g_send.at[t, q], g_recv.at[t, q], pair)

    def last(t, q, h):
        piece = fin.at[h, t, q]
        return remote(piece, piece, h_send.at[t, q], h_recv.at[t, q], sib)

    def combine(t, q):
        for m in order:
            returned(t, q, m).wait_recv()
        flat = ret[t, q].reshape(rows, width)
        if t == 0:
            flat = (flat.astype(F32) * slot_weight).astype(BF16)
        part[t, q] = mm(back, flat).astype(BF16)

        @pl.when(outer)
        def _():
            outward(t, q).start()

    def join(t, q):
        @pl.when(inner)
        def _():
            outward(t, q).wait_recv()
            joint[t, q] = (part[t, q].astype(F32) + from_outer[t, q].astype(F32)).astype(BF16)
            middle(t, q).start()

    def settle(t, q):
        @pl.when(inner)
        def _():
            middle(t, q).wait_recv()
            v = joint[t, q].astype(F32) + from_inner[t, q].astype(F32)
            fin[c, t, q] = v.astype(BF16)
            spread(t, q).start()
            last(t, q, c).start()

    def arrive(t, q):
        @pl.when(outer)
        def _():
            spread(t, q).wait_recv()
            last(t, q, c).start()

    def place(t, q):
        last(t, q, 1 - c).wait_recv()
        for h in range(2):
            at = h * half + q * width
            (output, input_grad)[t][:, at : at + width] = fin[h, t, q]

    def turn(k):
        for h in range(2):
            x = slots[h, 0].reshape(rows, half)
            step = half // chunks
            x_turned[h * half + k * step : h * half + (k + 1) * step] = x[
                :, k * step : (k + 1) * step
            ].T
        if k < 2:
            dy_rows[:, k * half : (k + 1) * half] = slots[k, 1].reshape(rows, half)
        if k == chunks - 1:
            hid_turned[...] = hid[...].T

    beat = 8.4 * width / half
    hop = beat + 1.7
    todo = []
    for t in range(2):
        for q in range(chunks):
            at = beat * (t * chunks + q)
            for i, act in enumerate((combine, join, settle, arrive, place)):
                todo.append((at + i * hop, i, t, q, act))
    for _, i, t, q, act in sorted(todo, key=lambda e: e[:4]):
        with jax.named_scope(f"{act.__name__}{t}{q}"):
            act(t, q)
            if i == 0 and t == 0:
                turn(q)

    for _, cp in sends:
        cp.wait_send()
    for t in range(2):
        for q in range(chunks):
            last(t, q, c).wait_send()

            @pl.when(outer)
            def _():
                outward(t, q).wait_send()

            @pl.when(inner)
            def _():
                middle(t, q).wait_send()
                spread(t, q).wait_send()


def grads_kernel(
    step, output, input_grad, x_turned, dy_rows, hid_turned, hid_dy,
    output_hbm, input_grad_hbm, gate_hbm, up_hbm, down_hbm,
    gate, up, down, sem, g_sem,
):
    copies = [
        pltpu.make_async_copy(output, output_hbm, sem.at[0]),
        pltpu.make_async_copy(input_grad, input_grad_hbm, sem.at[1]),
    ]
    for cp in copies:
        cp.start()
    features = x_turned.shape[0]
    units = hid_turned.shape[0]

    def emit(k, at, value, buf, dst):
        buf[pl.ds(at, value.shape[0])] = value.astype(BF16)
        cp = pltpu.make_async_copy(
            buf.at[pl.ds(at, value.shape[0])], dst.at[pl.ds(at, value.shape[0])], g_sem.at[k]
        )
        cp.start()
        copies.append(cp)

    k = 0
    for at in range(0, features, step):
        x = x_turned[at : at + step]
        emit(k, at, mm(x, hid_dy[0]), gate, gate_hbm)
        emit(k + 1, at, mm(x, hid_dy[1]), up, up_hbm)
        k += 2
    rows_at = min(256, units)
    for at in range(0, units, rows_at):
        emit(k, at, mm(hid_turned[at : at + rows_at], dy_rows[...]), down, down_hbm)
        k += 1
    for cp in copies:
        cp.wait()


def fused(tokens, cotangent, routes, router_weight, w_gate, w_up, w_down):
    n = lax.axis_size("dp")
    toks, features = tokens.shape
    cap = capacity_of(toks, n)
    rows = n * cap
    half = features // 2
    units = w_gate.shape[2]
    tile = 512
    wide = 768
    width = 256
    chunks = half // width
    vmem = pl.BlockSpec(memory_space=pltpu.VMEM)
    hbm = pl.BlockSpec(memory_space=pl.ANY)
    dma = pltpu.SemaphoreType.DMA
    V = pltpu.VMEM
    held = pl.pallas_call(
        functools.partial(routed_kernel, n, cap, tile, wide, width),
        out_shape=(
            V((toks, features), BF16),
            V((toks, features), BF16),
            V((features, rows), BF16),
            V((rows, features), BF16),
            V((units, rows), BF16),
            V((2, rows, units), BF16),
        ),
        in_specs=[hbm] * 7,
        out_specs=(vmem,) * 6,
        scratch_shapes=[
            V((toks, features), BF16),
            V((toks, features), BF16),
            V((2, toks), jnp.int32),
            V((2, toks), F32),
            V((features, units), BF16),
            V((features, units), BF16),
            V((units, features), BF16),
            V((2, 2, n, cap, half), BF16),
            V((2, n, cap, half), BF16),
            V((rows, units), F32),
            V((rows, units), F32),
            V((rows, units), BF16),
            V((2, chunks, n, cap, width), BF16),
            V((2, chunks, n, cap, width), BF16),
            V((2, half // wide, rows, wide), F32),
            V((2, chunks, n, cap, width), BF16),
            V((2, chunks, n, cap, width), BF16),
            V((2, chunks, toks, width), BF16),
            V((2, chunks, toks, width), BF16),
            V((2, chunks, toks, width), BF16),
            V((2, chunks, toks, width), BF16),
            V((2, 2, chunks, toks, width), BF16),
            dma((7,)),
            dma((2, n)), dma((2, n)), dma((2,)), dma((2,)),
            dma((2, n + 1)), dma((2, n + 1)),
            dma((2, chunks)), dma((2, chunks)),
            dma((2, chunks, n)), dma((2, chunks, n)),
            dma((2, chunks)), dma((2, chunks)), dma((2, chunks)), dma((2, chunks)),
            dma((2, chunks)), dma((2, chunks)), dma((2, chunks)), dma((2, chunks)),
        ],
        compiler_params=pltpu.CompilerParams(
            collective_id=0, has_side_effects=True, vmem_limit_bytes=54 * 1000 * 1000
        ),
        name="routed",
    )(tokens, cotangent, routes.T, router_weight.T, w_gate[0], w_up[0], w_down[0])

    step = 512
    output, input_grad, grad_gate, grad_up, grad_down = pl.pallas_call(
        functools.partial(grads_kernel, step),
        out_shape=(
            jax.ShapeDtypeStruct((toks, features), BF16),
            jax.ShapeDtypeStruct((toks, features), BF16),
            jax.ShapeDtypeStruct((features, units), BF16),
            jax.ShapeDtypeStruct((features, units), BF16),
            jax.ShapeDtypeStruct((units, features), BF16),
        ),
        in_specs=[vmem] * 6,
        out_specs=(hbm,) * 5,
        scratch_shapes=[
            V((features, units), BF16),
            V((features, units), BF16),
            V((units, features), BF16),
            dma((2,)),
            dma((2 * features // step + units // min(256, units),)),
        ],
        compiler_params=pltpu.CompilerParams(vmem_limit_bytes=50 * 1000 * 1000),
        name="grads",
    )(*held)
    return output, input_grad, grad_gate[None], grad_up[None], grad_down[None]


def slot_tables(routes, router_weight, experts, capacity):
    expert_ids = jnp.arange(experts, dtype=jnp.int32)
    hit_table = (routes[:, :, None] == expert_ids).astype(jnp.int32)
    per_token = jnp.sum(hit_table, axis=1)
    before = jnp.cumsum(per_token, axis=0) - per_token
    slot_of = jnp.sum(hit_table * before[:, None, :], axis=2)
    slot_ids = jnp.arange(capacity, dtype=jnp.int32)
    placed = hit_table[:, :, :, None] * (slot_of[:, :, None, None] == slot_ids).astype(jnp.int32)
    tok_rows = routes.shape[0]
    flat = placed.reshape(tok_rows, 2, experts * capacity).astype(jnp.float32)
    slot_weight = jnp.sum(flat * router_weight[:, :, None], axis=(0, 1))
    return (flat[:, 0], flat[:, 1], slot_weight)


def on_device(tokens, cotangent, routes, router_weight, w_gate, w_up, w_down):
    experts = lax.axis_size("dp")
    tok_rows, features = tokens.shape
    capacity = max(tok_rows * 3 // 8, tok_rows * 2 // experts, 2)
    local_rows = experts * capacity
    lead = (((0,), (0,)), ((), ()))
    trail = (((1,), (1,)), ((), ()))
    first_pick, second_pick, slot_weight = slot_tables(routes, router_weight, experts, capacity)
    picked = (first_pick + second_pick).astype(jnp.bfloat16)
    send_x = lax.dot_general(picked, tokens, lead, preferred_element_type=jnp.float32).astype(
        jnp.bfloat16
    )
    chosen_dy = lax.dot_general(picked, cotangent, lead, preferred_element_type=jnp.float32)
    send_dy = (chosen_dy * slot_weight[:, None]).astype(jnp.bfloat16)
    arrived_x, arrived_dy = (
        lax.all_to_all(
            send_x.reshape(experts, capacity, features),
            "dp",
            split_axis=0,
            concat_axis=0,
            tiled=True,
        ),
        lax.all_to_all(
            send_dy.reshape(experts, capacity, features),
            "dp",
            split_axis=0,
            concat_axis=0,
            tiled=True,
        ),
    )
    slot_x = arrived_x.reshape(local_rows, features)
    slot_dy = arrived_dy.reshape(local_rows, features)
    gate_w = w_gate[0]
    up_w = w_up[0]
    down_w = w_down[0]
    gate_pre = jnp.dot(slot_x, gate_w, preferred_element_type=jnp.float32)
    up_pre = jnp.dot(slot_x, up_w, preferred_element_type=jnp.float32)
    sigma = jax.nn.sigmoid(gate_pre)
    active = gate_pre * sigma
    hidden = (active * up_pre).astype(jnp.bfloat16)
    out_terms = jnp.dot(hidden, down_w, preferred_element_type=jnp.float32)
    hidden_dy = lax.dot_general(slot_dy, down_w, trail, preferred_element_type=jnp.float32)
    gate_dy = (hidden_dy * up_pre * sigma * (1.0 + gate_pre * (1.0 - sigma))).astype(jnp.bfloat16)
    up_dy = (hidden_dy * active).astype(jnp.bfloat16)
    grad_down = lax.dot_general(hidden, slot_dy, lead, preferred_element_type=jnp.float32).astype(
        jnp.bfloat16
    )
    grad_gate = lax.dot_general(slot_x, gate_dy, lead, preferred_element_type=jnp.float32).astype(
        jnp.bfloat16
    )
    grad_up = lax.dot_general(slot_x, up_dy, lead, preferred_element_type=jnp.float32).astype(
        jnp.bfloat16
    )
    back_terms = lax.dot_general(
        gate_dy, gate_w, trail, preferred_element_type=jnp.float32
    ) + lax.dot_general(up_dy, up_w, trail, preferred_element_type=jnp.float32)
    out_part, back_part = (
        lax.psum_scatter(
            out_terms.reshape(experts, capacity, features).astype(jnp.bfloat16),
            "fsdp",
            scatter_dimension=2,
            tiled=True,
        ).astype(jnp.float32),
        lax.psum_scatter(
            back_terms.reshape(experts, capacity, features).astype(jnp.bfloat16),
            "fsdp",
            scatter_dimension=2,
            tiled=True,
        ).astype(jnp.float32),
    )
    returned_out, returned_dx = (
        lax.all_to_all(
            out_part.astype(jnp.bfloat16), "dp", split_axis=0, concat_axis=0, tiled=True
        ),
        lax.all_to_all(
            back_part.astype(jnp.bfloat16), "dp", split_axis=0, concat_axis=0, tiled=True
        ),
    )
    width = out_part.shape[2]
    flat_out = returned_out.reshape(local_rows, width)
    flat_dx = returned_dx.reshape(local_rows, width)
    first_rows = jnp.dot(
        first_pick.astype(jnp.bfloat16), flat_out, preferred_element_type=jnp.float32
    )
    second_rows = jnp.dot(
        second_pick.astype(jnp.bfloat16), flat_out, preferred_element_type=jnp.float32
    )
    output = (router_weight[:, 0:1] * first_rows + router_weight[:, 1:2] * second_rows).astype(
        jnp.bfloat16
    )
    input_grad = jnp.dot(picked, flat_dx, preferred_element_type=jnp.float32).astype(jnp.bfloat16)
    output, input_grad = (
        lax.all_gather(output, "fsdp", axis=1, tiled=True),
        lax.all_gather(input_grad, "fsdp", axis=1, tiled=True),
    )
    return (output, input_grad, grad_gate[None], grad_up[None], grad_down[None])


def capacity_of(toks, experts):
    return max(toks * 3 // 8, toks * 2 // experts, 2)


def fits(mesh, toks, features, units):
    n, m = mesh.shape["dp"], mesh.shape["fsdp"]
    cap = capacity_of(toks, n)
    lines = n == 4 and m == 8
    whole = features % 1536 == 0 and units % 512 == 0 and cap % 32 == 0 and toks % 128 == 0
    rows = n * cap
    held = 6 * features * units + 2 * rows * (15 * features + 8 * units) + 20 * toks * features
    return lines and whole and held < 56 * 1000 * 1000


def solution(mesh):
    def step(tokens, cotangent, routes, router_weight, w_gate, w_up, w_down):
        body = fused if fits(mesh, *tokens.shape, w_gate.shape[2]) else on_device
        return body(tokens, cotangent, routes, router_weight, w_gate, w_up, w_down)

    return jax.shard_map(
        step,
        mesh=mesh,
        in_specs=(
            P("dp", None),
            P("dp", None),
            P("dp", None),
            P("dp", None),
            P("dp", None, "fsdp"),
            P("dp", None, "fsdp"),
            P("dp", "fsdp", None),
        ),
        out_specs=(
            P("dp", None),
            P("dp", None),
            P("dp", None, "fsdp"),
            P("dp", None, "fsdp"),
            P("dp", "fsdp", None),
        ),
        check_vma=False,
    )
```

```python
import functools

import jax
import jax.numpy as jnp
from jax import lax
from jax.experimental import pallas as pl
from jax.experimental.pallas import tpu as pltpu
from jax.sharding import PartitionSpec as P

MESH = pl.DeviceIdType.MESH
BF16 = jnp.bfloat16
F32 = jnp.float32
LEAD = (((0,), (0,)), ((), ()))
TRAIL = (((1,), (1,)), ((), ()))


def flip(a, mask):
    bit = 1
    while bit <= mask:
        if mask & bit:
            a = a + bit - 2 * bit * ((a // bit) % 2)
        bit *= 2
    return a


def xor(v, a, n):
    out = v - v
    bit = 1
    while bit < n:
        x, y = (v // bit) % 2, (a // bit) % 2
        out = out + bit * (x + y - 2 * x * y)
        bit *= 2
    return out


def mm(a, b, dims=(((1,), (0,)), ((), ()))):
    return lax.dot_general(a, b, dims, preferred_element_type=F32)


def routed_kernel(
    n, cap, tile, wide, pieces,
    tokens_hbm, cotangent_hbm, routes_hbm, rweight_hbm, wg_hbm, wu_hbm, wd_hbm,
    output, input_grad, x_turned, dy_rows, hid_turned, hid_dy,
    tok, cot, rts, rwt, wg, wu, wd, slots, snd, gpre, upre, hacc, hid,
    core_snd, core_rcv, own, ret_snd, ret, part, from_outer, joint, from_inner, fin,
    w_sem, a_send, a_recv, d_send, d_recv, f_send, f_recv, c_send, c_recv, r_send, r_recv,
    s_send, s_recv, j_send, j_recv, h_send, h_recv,
):
    d = lax.axis_index("dp")
    f = lax.axis_index("fsdp")
    c = f % 2
    z = f // 2
    sib = (d, flip(f, 1))
    pair = (d, flip(f, 2))
    across = (d, 2 * (3 - z) + c)
    outer = (z % 3) == 0
    inner = (z % 3) != 0
    toks, features = tok.shape
    half = features // 2
    rows = n * cap
    units = gpre.shape[1]
    slabs = half // 128
    order = sorted(range(1, n), key=lambda m: -bin(m).count("1"))
    far = order[0]
    near = order[1:]
    share = cap // 2

    def remote(src, dst, ssem, rsem, dev):
        return pltpu.make_async_remote_copy(
            src_ref=src, dst_ref=dst, send_sem=ssem, recv_sem=rsem,
            device_id=dev, device_id_type=MESH,
        )

    barrier = pltpu.get_barrier_semaphore()
    friends = [(flip(d, m), f) for m in order] + [sib, pair, across]
    for dev in friends:
        pl.semaphore_signal(barrier, inc=1, device_id=dev, device_id_type=MESH)

    loads = [
        pltpu.make_async_copy(s, t, w_sem.at[k])
        for k, (s, t) in enumerate(
            (
                (routes_hbm, rts), (rweight_hbm, rwt), (tokens_hbm, tok), (cotangent_hbm, cot),
                (wg_hbm, wg), (wu_hbm, wu), (wd_hbm, wd),
            )
        )
    ]
    for load in loads:
        load.start()
    with jax.named_scope('w_small'):
        loads[0].wait()
        loads[1].wait()

    slot_row = lax.broadcasted_iota(jnp.int32, (rows, toks), 0)
    m_of = slot_row // cap
    e_of = xor(m_of, d, n)
    s_of = (slot_row % cap).astype(F32)
    r = rts[...]
    hit0 = r[0:1, :] == e_of
    hit1 = r[1:2, :] == e_of
    per_token = jnp.where(hit0 | hit1, 1.0, 0.0).astype(BF16)
    earlier = (
        lax.broadcasted_iota(jnp.int32, (toks, toks), 0)
        < lax.broadcasted_iota(jnp.int32, (toks, toks), 1)
    )
    before = mm(per_token, jnp.where(earlier, 1.0, 0.0).astype(BF16))
    here = before == s_of
    first = jnp.where(hit0 & here, 1.0, 0.0)
    second = jnp.where(hit1 & here, 1.0, 0.0)
    rw = rwt[...]
    slot_weight = jnp.sum(first * rw[0:1, :] + second * rw[1:2, :], axis=1, keepdims=True)
    picked = (first + second).astype(BF16)
    same = (
        lax.broadcasted_iota(jnp.int32, (toks, toks), 0)
        == lax.broadcasted_iota(jnp.int32, (toks, toks), 1)
    )
    back = mm(jnp.where(same, 1.0, 0.0).astype(BF16), picked, TRAIL).astype(BF16)

    mine = pl.ds(pl.multiple_of(c * half, 128), half)
    other = pl.ds(pl.multiple_of((1 - c) * half, 128), half)

    def build(t):
        src = (tok, cot)[t]
        v = mm(picked, src[:, mine])
        u = mm(picked[:cap], src[:, other])
        if t:
            v = v * slot_weight
            u = u * slot_weight[:cap]
        snd[t] = v.astype(BF16).reshape(n, cap, half)
        slots[c, t, 0] = v[:cap].astype(BF16)
        slots[1 - c, t, 0] = u.astype(BF16)

    held = pl.ds(pl.multiple_of((z % 2) * share, 16), share)
    missing = pl.ds(pl.multiple_of((1 - z % 2) * share, 16), share)
    parts = 2
    depth = half // parts

    def part_of(j):
        return pl.ds(j * depth, depth)

    def direct(t, m, j):
        dev = (flip(d, m), f)
        if m == far:
            return remote(
                snd.at[t, m, held, part_of(j)], slots.at[c, t, m, held, part_of(j)],
                a_send.at[t, 0], a_recv.at[t, j, 0], dev,
            )
        return remote(
            snd.at[t, m, :, part_of(j)], slots.at[c, t, m, :, part_of(j)],
            a_send.at[t, 1], a_recv.at[t, j, m], dev,
        )

    def dispatch(t):
        for j in range(parts):
            direct(t, far, j).start()
        for j in range(parts):
            for m in near:
                direct(t, m, j).start()

    def relay(t, j, rows_at):
        piece = slots.at[c, t, far, rows_at, part_of(j)]
        return remote(piece, piece, d_send.at[t], d_recv.at[t, j], pair)

    def forward(t, j, k):
        if k == 0:
            piece = slots.at[c, t, far, held, part_of(j)]
        elif k == n:
            piece = slots.at[c, t, far, missing, part_of(j)]
        else:
            piece = slots.at[c, t, k, :, part_of(j)]
        return remote(piece, piece, f_send.at[t], f_recv.at[t, j], sib)

    def relay_far(t, j):
        direct(t, far, j).wait_recv()
        relay(t, j, held).start()
        forward(t, j, 0).start()

    def collect(t, j):
        for m in near:
            direct(t, m, j).wait_recv()
            forward(t, j, m).start()
        relay(t, j, missing).wait_recv()
        forward(t, j, n).start()

    def collected(t, j):
        theirs = slots.at[1 - c, t, pl.ds(1, n - 1), :, part_of(j)]
        remote(theirs, theirs, f_send.at[t], f_recv.at[t, j], sib).wait_recv()

    loads[2].wait()
    with jax.named_scope("build0"):
        build(0)
    with jax.named_scope("w_barrier"):
        pl.semaphore_wait(barrier, len(friends))
    dispatch(0)
    loads[3].wait()
    with jax.named_scope("build1"):
        build(1)
    dispatch(1)

    def at_half(h):
        return pl.ds(pl.multiple_of(h * half, 128), half)

    def activate(at, cols, g, u):
        gpre[at, cols] = g
        upre[at, cols] = u
        hid[at, cols] = (g * jax.nn.sigmoid(g) * u).astype(BF16)

    self_rows = pl.ds(0, cap)
    their_rows = pl.ds(cap, rows - cap)

    def self_gate(j, carry):
        cols = pl.ds(j * tile, tile)
        gpre[self_rows, cols] = mm(slots[0, 0, 0], wg[pl.ds(0, half), cols]) + mm(
            slots[1, 0, 0], wg[pl.ds(half, half), cols]
        )
        return carry

    def self_up(j, carry):
        cols = pl.ds(j * tile, tile)
        u = mm(slots[0, 0, 0], wu[pl.ds(0, half), cols]) + mm(
            slots[1, 0, 0], wu[pl.ds(half, half), cols]
        )
        activate(self_rows, cols, gpre[self_rows, cols], u)
        return carry

    def near_part(h, k, j, carry):
        cols = pl.ds(j * tile, tile)
        x = slots[h, 0, 1:, :, part_of(k)].reshape(rows - cap, depth)
        at = pl.ds(pl.multiple_of(h * half + k * depth, 128), depth)
        gpre[their_rows, cols] += mm(x, wg[at, cols])
        upre[their_rows, cols] += mm(x, wu[at, cols])
        return carry

    def first_part(j, carry):
        cols = pl.ds(j * tile, tile)
        x = slots[c, 0, 1:, :, part_of(0)].reshape(rows - cap, depth)
        at = pl.ds(pl.multiple_of(c * half, 128), depth)
        gpre[their_rows, cols] = mm(x, wg[at, cols])
        upre[their_rows, cols] = mm(x, wu[at, cols])
        return carry

    def last_part(j, carry):
        cols = pl.ds(j * tile, tile)
        x = slots[1 - c, 0, 1:, :, part_of(parts - 1)].reshape(rows - cap, depth)
        at = pl.ds(pl.multiple_of((1 - c) * half + (parts - 1) * depth, 128), depth)
        g = gpre[their_rows, cols] + mm(x, wg[at, cols])
        u = upre[their_rows, cols] + mm(x, wu[at, cols])
        activate(their_rows, cols, g, u)
        return carry

    def each_tile(body):
        for j in range(units // tile):
            body(j, 0)

    loads[4].wait()
    with jax.named_scope("self_gate"):
        each_tile(self_gate)
    loads[5].wait()
    with jax.named_scope("self_up"):
        each_tile(self_up)
    with jax.named_scope("relay0"):
        relay_far(0, 0)
        relay_far(0, 1)
    with jax.named_scope("collect00"):
        collect(0, 0)
    with jax.named_scope("own0"):
        each_tile(first_part)
    with jax.named_scope("collect01"):
        collect(0, 1)
    with jax.named_scope("own1"):
        each_tile(functools.partial(near_part, c, 1))
    with jax.named_scope("collected00"):
        collected(0, 0)
    with jax.named_scope("relay10"):
        relay_far(1, 0)
    with jax.named_scope("sib0"):
        each_tile(functools.partial(near_part, 1 - c, 0))
    with jax.named_scope("collected01"):
        collected(0, 1)
    with jax.named_scope("relay11"):
        relay_far(1, 1)
    with jax.named_scope("sib1"):
        each_tile(last_part)
    loads[6].wait()

    def swap(t, k):
        return remote(core_snd.at[t, k], core_rcv.at[t, k], c_send.at[t], c_recv.at[t, k], sib)

    def returned(t, q, m):
        at = pl.ds(*pieces[t][q])
        return remote(
            ret_snd.at[t, at, m], ret.at[t, at, m], r_send.at[t], r_recv.at[t, q], (flip(d, m), f)
        )

    per = wide // 128

    def term(t, cols):
        if t == 0:
            return mm(hid[...], wd[:, cols])
        return mm(hid_dy[0], wg[cols, :], TRAIL) + mm(hid_dy[1], wu[cols, :], TRAIL)

    def theirs(t, k):
        at = pl.multiple_of((1 - c) * half + k * wide, 128)
        core_snd[t, k] = term(t, pl.ds(at, wide)).astype(BF16)
        swap(t, k).start()

    def ours(t, k):
        at = pl.multiple_of(c * half + k * wide, 128)
        own[t, k] = term(t, pl.ds(at, wide))

    def finish(t, k):
        swap(t, k).wait_recv()
        for q, (g0, count) in enumerate(pieces[t]):
            if g0 // per != k:
                continue
            for m in order + [0]:
                for g in range(g0, g0 + count):
                    at = (g - k * per) * 128
                    rows_at = pl.ds(m * cap, cap)
                    v = own[t, k, rows_at, at : at + 128] + core_rcv[
                        t, k, rows_at, at : at + 128
                    ].astype(F32)
                    (ret_snd if m else ret)[t, g, m] = v.astype(BF16)
                if m:
                    returned(t, q, m).start()

    def down_own():
        def body(j, carry):
            cols = pl.ds(j * tile, tile)
            hacc[:, cols] = mm(slots[c, 1].reshape(rows, half), wd[cols, mine], TRAIL)
            return carry

        each_tile(body)

    def down_rest():
        def body(j, carry):
            cols = pl.ds(j * tile, tile)
            hdy = hacc[:, cols] + mm(slots[1 - c, 1].reshape(rows, half), wd[cols, other], TRAIL)
            g = gpre[:, cols]
            sig = jax.nn.sigmoid(g)
            hid_dy[0, :, cols] = (hdy * upre[:, cols] * sig * (1.0 + g * (1.0 - sig))).astype(BF16)
            hid_dy[1, :, cols] = (hdy * (g * sig)).astype(BF16)
            return carry

        each_tile(body)

    def outward(t, q):
        at = pl.ds(*pieces[t][q])
        return remote(part.at[t, at], from_outer.at[t, at], s_send.at[t], s_recv.at[t, q], pair)

    def middle(t, q):
        at = pl.ds(*pieces[t][q])
        return remote(joint.at[t, at], from_inner.at[t, at], j_send.at[t], j_recv.at[t, q], across)

    def spread(t, q):
        piece = fin.at[c, t, pl.ds(*pieces[t][q])]
        return remote(piece, piece, s_send.at[t], s_recv.at[t, q], pair)

    def last(t, q, h):
        piece = fin.at[h, t, pl.ds(*pieces[t][q])]
        return remote(piece, piece, h_send.at[t], h_recv.at[t, q], sib)

    def combine(t, q):
        g0, count = pieces[t][q]
        landed = ret.at[t, pl.ds(g0, count), pl.ds(1, n - 1)]
        remote(landed, landed, r_send.at[t], r_recv.at[t, q], sib).wait_recv()
        flat = jnp.concatenate([ret[t, g].reshape(rows, 128) for g in range(g0, g0 + count)], axis=1)
        if t == 0:
            flat = (flat.astype(F32) * slot_weight).astype(BF16)
        v = mm(back, flat).astype(BF16)
        for i in range(count):
            part[t, g0 + i] = v[:, i * 128 : (i + 1) * 128]

        @pl.when(outer)
        def _():
            outward(t, q).start()

    def join(t, q):
        at = pl.ds(*pieces[t][q])

        @pl.when(inner)
        def _():
            outward(t, q).wait_recv()
            joint[t, at] = (part[t, at].astype(F32) + from_outer[t, at].astype(F32)).astype(BF16)
            middle(t, q).start()

    def settle(t, q):
        at = pl.ds(*pieces[t][q])

        @pl.when(inner)
        def _():
            middle(t, q).wait_recv()
            v = joint[t, at].astype(F32) + from_inner[t, at].astype(F32)
            fin[c, t, at] = v.astype(BF16)
            spread(t, q).start()
            last(t, q, c).start()

    def arrive(t, q):
        @pl.when(outer)
        def _():
            spread(t, q).wait_recv()
            last(t, q, c).start()

    def place(t, q):
        last(t, q, 1 - c).wait_recv()
        g0, count = pieces[t][q]
        for h in range(2):
            for g in range(g0, g0 + count):
                at = h * half + g * 128
                (output, input_grad)[t][:, at : at + 128] = fin[h, t, g]

    def turn(k):
        h, i = k // 3, k % 3
        step = half // 3
        x = slots[h, 0].reshape(rows, half)[:, i * step : (i + 1) * step]
        x_turned[h * half + i * step : h * half + (i + 1) * step] = x.T
        if i == 0:
            dy_rows[:, h * half : (h + 1) * half] = slots[h, 1].reshape(rows, half)
        if k == 5:
            hid_turned[...] = hid[...].T

    def gather():
        for j in range(parts):
            collect(1, j)

    def gathered():
        for j in range(parts):
            collected(1, j)

    count = half // wide
    plan = []

    def at(when, what, *args):
        plan.append((when, len(plan), what, args))

    def project(t, when, unit, end):
        for k in range(count):
            at(when + 2 * k * unit, theirs, t, k)
            if k:
                at(when + 2 * k * unit + 0.01, finish, t, k - 1)
            at(when + (2 * k + 1) * unit, ours, t, k)
        at(end, finish, t, count - 1)

    beat = 0.7
    lag = 2.3
    project(0, 0.0, 0.46, 4.2)
    at(2.9, gather)
    at(3.0, down_own)
    at(4.25, gathered)
    at(4.3, down_rest)
    project(1, 5.6, 0.76, 11.2)
    for k in range(6):
        at(12.0 + k, turn, k)
    free = [0.0] * 4
    ready = [1.5, 8.2]
    for t in range(2):
        for q, (g0, size) in enumerate(pieces[t]):
            when = ready[t]
            for i, act in enumerate((combine, join, settle, arrive)):
                free[i] = max(free[i], when) + beat * size
                when = free[i] + lag + (1.0 if i == 0 else 0.0)
                at(when + (1.5 if act is arrive else 0.0), act, t, q)
            at(when + 2.8, place, t, q)
    for _, _, what, args in sorted(plan, key=lambda e: e[:2]):
        with jax.named_scope(what.__name__ + "".join(str(a) for a in args)):
            what(*args)

    with jax.named_scope("drain"):
        for t in range(2):
            sent = snd.at[t, far, held]
            remote(sent, sent, a_send.at[t, 0], a_recv.at[t, 0, 0], sib).wait_send()
            sent = snd.at[t, pl.ds(near[0], len(near))]
            remote(sent, sent, a_send.at[t, 1], a_recv.at[t, 0, 1], sib).wait_send()
            sent = slots.at[c, t, far, held]
            remote(sent, sent, d_send.at[t], d_recv.at[t, 0], pair).wait_send()
            sent = slots.at[c, t, pl.ds(1, n - 1)]
            remote(sent, sent, f_send.at[t], f_recv.at[t, 0], sib).wait_send()
            remote(core_snd.at[t], core_rcv.at[t], c_send.at[t], c_recv.at[t, 0], sib).wait_send()
            sent = ret_snd.at[t, :, pl.ds(1, n - 1)]
            remote(sent, sent, r_send.at[t], r_recv.at[t, 0], sib).wait_send()
            sent = fin.at[c, t]
            remote(sent, sent, h_send.at[t], h_recv.at[t, 0], sib).wait_send()

            @pl.when(outer)
            def _():
                sent = part.at[t]
                remote(sent, sent, s_send.at[t], s_recv.at[t, 0], pair).wait_send()

            @pl.when(inner)
            def _():
                sent = joint.at[t]
                remote(sent, sent, j_send.at[t], j_recv.at[t, 0], across).wait_send()
                sent = fin.at[c, t]
                remote(sent, sent, s_send.at[t], s_recv.at[t, 0], pair).wait_send()


def grads_kernel(
    step, output, input_grad, x_turned, dy_rows, hid_turned, hid_dy,
    output_hbm, input_grad_hbm, gate_hbm, up_hbm, down_hbm,
    gate, up, down, sem, g_sem,
):
    copies = [
        pltpu.make_async_copy(output, output_hbm, sem.at[0]),
        pltpu.make_async_copy(input_grad, input_grad_hbm, sem.at[1]),
    ]
    for cp in copies:
        cp.start()
    features = x_turned.shape[0]
    units = hid_turned.shape[0]

    def emit(k, at, value, buf, dst):
        buf[pl.ds(at, value.shape[0])] = value.astype(BF16)
        cp = pltpu.make_async_copy(
            buf.at[pl.ds(at, value.shape[0])], dst.at[pl.ds(at, value.shape[0])], g_sem.at[k]
        )
        cp.start()
        copies.append(cp)

    k = 0
    for at in range(0, features, step):
        x = x_turned[at : at + step]
        emit(k, at, mm(x, hid_dy[0]), gate, gate_hbm)
        emit(k + 1, at, mm(x, hid_dy[1]), up, up_hbm)
        k += 2
    rows_at = min(256, units)
    for at in range(0, units, rows_at):
        emit(k, at, mm(hid_turned[at : at + rows_at], dy_rows[...]), down, down_hbm)
        k += 1
    for cp in copies:
        cp.wait()


def fused(tokens, cotangent, routes, router_weight, w_gate, w_up, w_down):
    n = lax.axis_size("dp")
    toks, features = tokens.shape
    cap = capacity_of(toks, n)
    rows = n * cap
    half = features // 2
    units = w_gate.shape[2]
    tile = 512
    wide = 512
    slabs = half // 128
    even = [(g, 2) for g in range(0, slabs, 2)]
    pieces = ([(0, 1), (1, 1)] + even[1:], even[:-1] + [(slabs - 2, 1), (slabs - 1, 1)])
    most = max(len(p) for p in pieces)
    vmem = pl.BlockSpec(memory_space=pltpu.VMEM)
    hbm = pl.BlockSpec(memory_space=pl.ANY)
    dma = pltpu.SemaphoreType.DMA
    V = pltpu.VMEM
    held = pl.pallas_call(
        functools.partial(routed_kernel, n, cap, tile, wide, pieces),
        out_shape=(
            V((toks, features), BF16),
            V((toks, features), BF16),
            V((features, rows), BF16),
            V((rows, features), BF16),
            V((units, rows), BF16),
            V((2, rows, units), BF16),
        ),
        in_specs=[hbm] * 7,
        out_specs=(vmem,) * 6,
        scratch_shapes=[
            V((toks, features), BF16),
            V((toks, features), BF16),
            V((2, toks), jnp.int32),
            V((2, toks), F32),
            V((features, units), BF16),
            V((features, units), BF16),
            V((units, features), BF16),
            V((2, 2, n, cap, half), BF16),
            V((2, n, cap, half), BF16),
            V((rows, units), F32),
            V((rows, units), F32),
            V((rows, units), F32),
            V((rows, units), BF16),
            V((2, half // wide, rows, wide), BF16),
            V((2, half // wide, rows, wide), BF16),
            V((2, half // wide, rows, wide), F32),
            V((2, slabs, n, cap, 128), BF16),
            V((2, slabs, n, cap, 128), BF16),
            V((2, slabs, toks, 128), BF16),
            V((2, slabs, toks, 128), BF16),
            V((2, slabs, toks, 128), BF16),
            V((2, slabs, toks, 128), BF16),
            V((2, 2, slabs, toks, 128), BF16),
            dma((7,)),
            dma((2, 2)), dma((2, 2, n - 1)), dma((2,)), dma((2, 2)),
            dma((2,)), dma((2, 2)),
            dma((2,)), dma((2, half // wide)),
            dma((2,)), dma((2, most)),
            dma((2,)), dma((2, most)), dma((2,)), dma((2, most)), dma((2,)), dma((2, most)),
        ],
        compiler_params=pltpu.CompilerParams(
            collective_id=0, has_side_effects=True, vmem_limit_bytes=54 * 1000 * 1000
        ),
        name="routed",
    )(tokens, cotangent, routes.T, router_weight.T, w_gate[0], w_up[0], w_down[0])

    step = 512
    output, input_grad, grad_gate, grad_up, grad_down = pl.pallas_call(
        functools.partial(grads_kernel, step),
        out_shape=(
            jax.ShapeDtypeStruct((toks, features), BF16),
            jax.ShapeDtypeStruct((toks, features), BF16),
            jax.ShapeDtypeStruct((features, units), BF16),
            jax.ShapeDtypeStruct((features, units), BF16),
            jax.ShapeDtypeStruct((units, features), BF16),
        ),
        in_specs=[vmem] * 6,
        out_specs=(hbm,) * 5,
        scratch_shapes=[
            V((features, units), BF16),
            V((features, units), BF16),
            V((units, features), BF16),
            dma((2,)),
            dma((2 * features // step + units // min(256, units),)),
        ],
        compiler_params=pltpu.CompilerParams(vmem_limit_bytes=50 * 1000 * 1000),
        name="grads",
    )(*held)
    return output, input_grad, grad_gate[None], grad_up[None], grad_down[None]


def slot_tables(routes, router_weight, experts, capacity):
    expert_ids = jnp.arange(experts, dtype=jnp.int32)
    hit_table = (routes[:, :, None] == expert_ids).astype(jnp.int32)
    per_token = jnp.sum(hit_table, axis=1)
    before = jnp.cumsum(per_token, axis=0) - per_token
    slot_of = jnp.sum(hit_table * before[:, None, :], axis=2)
    slot_ids = jnp.arange(capacity, dtype=jnp.int32)
    placed = hit_table[:, :, :, None] * (slot_of[:, :, None, None] == slot_ids).astype(jnp.int32)
    tok_rows = routes.shape[0]
    flat = placed.reshape(tok_rows, 2, experts * capacity).astype(jnp.float32)
    slot_weight = jnp.sum(flat * router_weight[:, :, None], axis=(0, 1))
    return (flat[:, 0], flat[:, 1], slot_weight)


def on_device(tokens, cotangent, routes, router_weight, w_gate, w_up, w_down):
    experts = lax.axis_size("dp")
    tok_rows, features = tokens.shape
    capacity = max(tok_rows * 3 // 8, tok_rows * 2 // experts, 2)
    local_rows = experts * capacity
    lead = (((0,), (0,)), ((), ()))
    trail = (((1,), (1,)), ((), ()))
    first_pick, second_pick, slot_weight = slot_tables(routes, router_weight, experts, capacity)
    picked = (first_pick + second_pick).astype(jnp.bfloat16)
    send_x = lax.dot_general(picked, tokens, lead, preferred_element_type=jnp.float32).astype(
        jnp.bfloat16
    )
    chosen_dy = lax.dot_general(picked, cotangent, lead, preferred_element_type=jnp.float32)
    send_dy = (chosen_dy * slot_weight[:, None]).astype(jnp.bfloat16)
    arrived_x, arrived_dy = (
        lax.all_to_all(
            send_x.reshape(experts, capacity, features),
            "dp",
            split_axis=0,
            concat_axis=0,
            tiled=True,
        ),
        lax.all_to_all(
            send_dy.reshape(experts, capacity, features),
            "dp",
            split_axis=0,
            concat_axis=0,
            tiled=True,
        ),
    )
    slot_x = arrived_x.reshape(local_rows, features)
    slot_dy = arrived_dy.reshape(local_rows, features)
    gate_w = w_gate[0]
    up_w = w_up[0]
    down_w = w_down[0]
    gate_pre = jnp.dot(slot_x, gate_w, preferred_element_type=jnp.float32)
    up_pre = jnp.dot(slot_x, up_w, preferred_element_type=jnp.float32)
    sigma = jax.nn.sigmoid(gate_pre)
    active = gate_pre * sigma
    hidden = (active * up_pre).astype(jnp.bfloat16)
    out_terms = jnp.dot(hidden, down_w, preferred_element_type=jnp.float32)
    hidden_dy = lax.dot_general(slot_dy, down_w, trail, preferred_element_type=jnp.float32)
    gate_dy = (hidden_dy * up_pre * sigma * (1.0 + gate_pre * (1.0 - sigma))).astype(jnp.bfloat16)
    up_dy = (hidden_dy * active).astype(jnp.bfloat16)
    grad_down = lax.dot_general(hidden, slot_dy, lead, preferred_element_type=jnp.float32).astype(
        jnp.bfloat16
    )
    grad_gate = lax.dot_general(slot_x, gate_dy, lead, preferred_element_type=jnp.float32).astype(
        jnp.bfloat16
    )
    grad_up = lax.dot_general(slot_x, up_dy, lead, preferred_element_type=jnp.float32).astype(
        jnp.bfloat16
    )
    back_terms = lax.dot_general(
        gate_dy, gate_w, trail, preferred_element_type=jnp.float32
    ) + lax.dot_general(up_dy, up_w, trail, preferred_element_type=jnp.float32)
    out_part, back_part = (
        lax.psum_scatter(
            out_terms.reshape(experts, capacity, features).astype(jnp.bfloat16),
            "fsdp",
            scatter_dimension=2,
            tiled=True,
        ).astype(jnp.float32),
        lax.psum_scatter(
            back_terms.reshape(experts, capacity, features).astype(jnp.bfloat16),
            "fsdp",
            scatter_dimension=2,
            tiled=True,
        ).astype(jnp.float32),
    )
    returned_out, returned_dx = (
        lax.all_to_all(
            out_part.astype(jnp.bfloat16), "dp", split_axis=0, concat_axis=0, tiled=True
        ),
        lax.all_to_all(
            back_part.astype(jnp.bfloat16), "dp", split_axis=0, concat_axis=0, tiled=True
        ),
    )
    width = out_part.shape[2]
    flat_out = returned_out.reshape(local_rows, width)
    flat_dx = returned_dx.reshape(local_rows, width)
    first_rows = jnp.dot(
        first_pick.astype(jnp.bfloat16), flat_out, preferred_element_type=jnp.float32
    )
    second_rows = jnp.dot(
        second_pick.astype(jnp.bfloat16), flat_out, preferred_element_type=jnp.float32
    )
    output = (router_weight[:, 0:1] * first_rows + router_weight[:, 1:2] * second_rows).astype(
        jnp.bfloat16
    )
    input_grad = jnp.dot(picked, flat_dx, preferred_element_type=jnp.float32).astype(jnp.bfloat16)
    output, input_grad = (
        lax.all_gather(output, "fsdp", axis=1, tiled=True),
        lax.all_gather(input_grad, "fsdp", axis=1, tiled=True),
    )
    return (output, input_grad, grad_gate[None], grad_up[None], grad_down[None])


def capacity_of(toks, experts):
    return max(toks * 3 // 8, toks * 2 // experts, 2)


def fits(mesh, toks, features, units):
    n, m = mesh.shape["dp"], mesh.shape["fsdp"]
    cap = capacity_of(toks, n)
    lines = n == 4 and m == 8
    whole = features % 1536 == 0 and units % 512 == 0 and cap % 32 == 0 and toks % 128 == 0
    rows = n * cap
    held = 6 * features * units + 2 * rows * (15 * features + 8 * units) + 20 * toks * features
    return lines and whole and held < 56 * 1000 * 1000


def solution(mesh):
    def step(tokens, cotangent, routes, router_weight, w_gate, w_up, w_down):
        body = fused if fits(mesh, *tokens.shape, w_gate.shape[2]) else on_device
        return body(tokens, cotangent, routes, router_weight, w_gate, w_up, w_down)

    return jax.shard_map(
        step,
        mesh=mesh,
        in_specs=(
            P("dp", None),
            P("dp", None),
            P("dp", None),
            P("dp", None),
            P("dp", None, "fsdp"),
            P("dp", None, "fsdp"),
            P("dp", "fsdp", None),
        ),
        out_specs=(
            P("dp", None),
            P("dp", None),
            P("dp", None, "fsdp"),
            P("dp", None, "fsdp"),
            P("dp", "fsdp", None),
        ),
        check_vma=False,
    )
```

```python
import functools

import jax
import jax.numpy as jnp
from jax import lax
from jax.experimental import pallas as pl
from jax.experimental.pallas import tpu as pltpu
from jax.sharding import PartitionSpec as P

MESH = pl.DeviceIdType.MESH
BF16 = jnp.bfloat16
F32 = jnp.float32
LEAD = (((0,), (0,)), ((), ()))
TRAIL = (((1,), (1,)), ((), ()))


def flip(a, mask):
    bit = 1
    while bit <= mask:
        if mask & bit:
            a = a + bit - 2 * bit * ((a // bit) % 2)
        bit *= 2
    return a


def xor(v, a, n):
    out = v - v
    bit = 1
    while bit < n:
        x, y = (v // bit) % 2, (a // bit) % 2
        out = out + bit * (x + y - 2 * x * y)
        bit *= 2
    return out


def mm(a, b, dims=(((1,), (0,)), ((), ()))):
    return lax.dot_general(a, b, dims, preferred_element_type=F32)


def routed_kernel(
    n, cap, tile, spans, pieces, shares,
    tokens_hbm, cotangent_hbm, routes_hbm, rweight_hbm, wg_hbm, wu_hbm, wd_hbm,
    output, input_grad, x_turned, dy_rows, hid_turned, hid_dy,
    tok, cot, rts, rwt, wg, wu, wd, slots, snd, gpre, upre, hacc, hid,
    core_snd, core_rcv, own, ret_snd, ret, part, from_outer, joint, from_inner, fin,
    w_sem, a_send, a_recv, d_send, d_recv, f_send, f_recv, c_send, c_recv, r_send, r_recv,
    s_send, s_recv, j_send, j_recv, h_send, h_recv, x_send, x_recv,
):
    d = lax.axis_index("dp")
    f = lax.axis_index("fsdp")
    c = f % 2
    z = f // 2
    sib = (d, flip(f, 1))
    pair = (d, flip(f, 2))
    across = (d, 2 * (3 - z) + c)
    skew = (d, flip(f, 3))
    outer = (z % 3) == 0
    inner = (z % 3) != 0
    toks, features = tok.shape
    half = features // 2
    rows = n * cap
    units = gpre.shape[1]
    slabs = half // 128
    order = sorted(range(1, n), key=lambda m: -bin(m).count("1"))
    far = order[0]
    near = order[1:]
    share = cap // 2

    def remote(src, dst, ssem, rsem, dev):
        return pltpu.make_async_remote_copy(
            src_ref=src, dst_ref=dst, send_sem=ssem, recv_sem=rsem,
            device_id=dev, device_id_type=MESH,
        )

    barrier = pltpu.get_barrier_semaphore()
    friends = [(flip(d, m), f) for m in order] + [sib, pair, across, skew]
    for dev in friends:
        pl.semaphore_signal(barrier, inc=1, device_id=dev, device_id_type=MESH)

    loads = [
        pltpu.make_async_copy(s, t, w_sem.at[k])
        for k, (s, t) in enumerate(
            (
                (routes_hbm, rts), (rweight_hbm, rwt), (tokens_hbm, tok), (cotangent_hbm, cot),
                (wg_hbm, wg), (wu_hbm, wu), (wd_hbm, wd),
            )
        )
    ]
    for load in loads:
        load.start()
    with jax.named_scope('w_small'):
        loads[0].wait()
        loads[1].wait()

    slot_row = lax.broadcasted_iota(jnp.int32, (rows, toks), 0)
    m_of = slot_row // cap
    e_of = xor(m_of, d, n)
    s_of = (slot_row % cap).astype(F32)
    r = rts[...]
    hit0 = r[0:1, :] == e_of
    hit1 = r[1:2, :] == e_of
    per_token = jnp.where(hit0 | hit1, 1.0, 0.0).astype(BF16)
    earlier = (
        lax.broadcasted_iota(jnp.int32, (toks, toks), 0)
        < lax.broadcasted_iota(jnp.int32, (toks, toks), 1)
    )
    before = mm(per_token, jnp.where(earlier, 1.0, 0.0).astype(BF16))
    here = before == s_of
    first = jnp.where(hit0 & here, 1.0, 0.0)
    second = jnp.where(hit1 & here, 1.0, 0.0)
    rw = rwt[...]
    slot_weight = jnp.sum(first * rw[0:1, :] + second * rw[1:2, :], axis=1, keepdims=True)
    picked = (first + second).astype(BF16)
    same = (
        lax.broadcasted_iota(jnp.int32, (toks, toks), 0)
        == lax.broadcasted_iota(jnp.int32, (toks, toks), 1)
    )
    back = mm(jnp.where(same, 1.0, 0.0).astype(BF16), picked, TRAIL).astype(BF16)

    mine = pl.ds(pl.multiple_of(c * half, 128), half)
    other = pl.ds(pl.multiple_of((1 - c) * half, 128), half)

    def build(t):
        src = (tok, cot)[t]
        v = mm(picked, src[:, mine])
        u = mm(picked[:cap], src[:, other])
        if t:
            v = v * slot_weight
            u = u * slot_weight[:cap]
        snd[t] = v.astype(BF16).reshape(n, cap, half)
        slots[c, t, 0] = v[:cap].astype(BF16)
        slots[1 - c, t, 0] = u.astype(BF16)

    held = pl.ds(pl.multiple_of((z % 2) * share, 16), share)
    missing = pl.ds(pl.multiple_of((1 - z % 2) * share, 16), share)
    parts = a_recv.shape[1]
    depth = half // parts

    def part_of(j):
        return pl.ds(j * depth, depth)

    def direct(t, m, j):
        dev = (flip(d, m), f)
        if m == far:
            return remote(
                snd.at[t, m, held, part_of(j)], slots.at[c, t, m, held, part_of(j)],
                a_send.at[t, 0], a_recv.at[t, j, 0], dev,
            )
        return remote(
            snd.at[t, m, :, part_of(j)], slots.at[c, t, m, :, part_of(j)],
            a_send.at[t, 1], a_recv.at[t, j, m], dev,
        )

    def dispatch(t):
        for j in range(parts):
            direct(t, far, j).start()
        for j in range(parts):
            for m in near:
                direct(t, m, j).start()

    def relay(t, j, rows_at):
        piece = slots.at[c, t, far, rows_at, part_of(j)]
        return remote(piece, piece, d_send.at[t], d_recv.at[t, j], pair)

    def forward(t, j, k):
        if k == 0:
            piece = slots.at[c, t, far, held, part_of(j)]
        elif k == n:
            piece = slots.at[c, t, far, missing, part_of(j)]
        else:
            piece = slots.at[c, t, k, :, part_of(j)]
        return remote(piece, piece, f_send.at[t], f_recv.at[t, j], sib)

    def relay_far(t, j):
        direct(t, far, j).wait_recv()
        relay(t, j, held).start()
        forward(t, j, 0).start()

    def collect(t, j):
        for m in near:
            direct(t, m, j).wait_recv()
            forward(t, j, m).start()
        relay(t, j, missing).wait_recv()
        forward(t, j, n).start()

    def collected(t, j):
        theirs = slots.at[1 - c, t, pl.ds(1, n - 1), :, part_of(j)]
        remote(theirs, theirs, f_send.at[t], f_recv.at[t, j], sib).wait_recv()

    loads[2].wait()
    with jax.named_scope("build0"):
        build(0)
    with jax.named_scope("w_barrier"):
        pl.semaphore_wait(barrier, len(friends))
    dispatch(0)
    loads[3].wait()
    with jax.named_scope("build1"):
        build(1)
    dispatch(1)

    def at_half(h):
        return pl.ds(pl.multiple_of(h * half, 128), half)

    def activate(at, cols, g, u):
        gpre[at, cols] = g
        upre[at, cols] = u
        hid[at, cols] = (g * jax.nn.sigmoid(g) * u).astype(BF16)

    def gate_up(m0, blocks, h, k, first=False, final=False):
        at = pl.ds(m0 * cap, blocks * cap)
        depth_at = pl.ds(pl.multiple_of(h * half + k * depth, 128), depth)
        for j in range(units // tile):
            cols = pl.ds(j * tile, tile)
            x = slots[h, 0, m0 : m0 + blocks, :, part_of(k)].reshape(blocks * cap, depth)
            g = mm(x, wg[depth_at, cols])
            u = mm(x, wu[depth_at, cols])
            if not first:
                g = g + gpre[at, cols]
                u = u + upre[at, cols]
            gpre[at, cols] = g
            upre[at, cols] = u
            if final:
                hid[at, cols] = (g * jax.nn.sigmoid(g) * u).astype(BF16)

    def scoped(what, *args, **kw):
        with jax.named_scope(what.__name__ + "".join(str(a) for a in args if isinstance(a, int))):
            what(*args, **kw)

    loads[4].wait()
    loads[5].wait()
    for i in range(2 * parts):
        scoped(
            gate_up, 0, 1, c if i < parts else 1 - c, i % parts,
            first=i == 0, final=i == 2 * parts - 1,
        )
    for j in range(parts):
        scoped(relay_far, 0, j)
    others = n - 1
    for j in range(parts):
        scoped(collect, 0, j)
        scoped(gate_up, 1, others, c, j, first=j == 0)
        if 0 < j < parts - 1:
            scoped(collected, 0, j - 1)
            scoped(gate_up, 1, others, 1 - c, j - 1)
    for j in range(max(0, parts - 2), parts):
        scoped(collected, 0, j)
        scoped(gate_up, 1, others, 1 - c, j, final=j == parts - 1)
        if j < parts - 1:
            for k in range(parts - 1):
                scoped(relay_far, 1, k)
    scoped(relay_far, 1, parts - 1)
    loads[6].wait()

    def span(t, k):
        return pl.ds(spans[t][k][0] * 128, spans[t][k][1] * 128)

    def swap(t, k):
        at = span(t, k)
        return remote(
            core_snd.at[t, :, at], core_rcv.at[t, :, at], c_send.at[t], c_recv.at[t, k], sib
        )

    def returned(t, q, m):
        at = pl.ds(*pieces[t][q])
        return remote(
            ret_snd.at[t, at, m], ret.at[t, at, m], r_send.at[t], r_recv.at[t, q], (flip(d, m), f)
        )

    def term(t, cols):
        if t == 0:
            return mm(hid[...], wd[:, cols])
        return mm(hid_dy[0], wg[cols, :], TRAIL) + mm(hid_dy[1], wu[cols, :], TRAIL)

    def theirs(t, k):
        g0, size = spans[t][k]
        at = pl.multiple_of((1 - c) * half + g0 * 128, 128)
        core_snd[t, :, span(t, k)] = term(t, pl.ds(at, size * 128)).astype(BF16)
        swap(t, k).start()

    def ours(t, k):
        g0, size = spans[t][k]
        at = pl.multiple_of(c * half + g0 * 128, 128)
        own[t, :, span(t, k)] = term(t, pl.ds(at, size * 128))

    def finish(t, k):
        swap(t, k).wait_recv()
        low, size = spans[t][k]
        for q, (g0, count) in enumerate(pieces[t]):
            if not low <= g0 < low + size:
                continue
            for m in order + [0]:
                for g in range(g0, g0 + count):
                    cols = pl.ds(g * 128, 128)
                    at = pl.ds(m * cap, cap)
                    v = own[t, at, cols] + core_rcv[t, at, cols].astype(F32)
                    (ret_snd if m else ret)[t, g, m] = v.astype(BF16)
                if m:
                    returned(t, q, m).start()

    def down_own():
        for j in range(units // tile):
            cols = pl.ds(j * tile, tile)
            hacc[:, cols] = mm(slots[c, 1].reshape(rows, half), wd[cols, mine], TRAIL)

    def down_rest(j):
        cols = pl.ds(j * tile, tile)
        hdy = hacc[:, cols] + mm(slots[1 - c, 1].reshape(rows, half), wd[cols, other], TRAIL)
        g = gpre[:, cols]
        sig = jax.nn.sigmoid(g)
        hid_dy[0, :, cols] = (hdy * upre[:, cols] * sig * (1.0 + g * (1.0 - sig))).astype(BF16)
        hid_dy[1, :, cols] = (hdy * (g * sig)).astype(BF16)

    def outward(t, g):
        return remote(part.at[t, g], from_outer.at[t, g], s_send.at[t], s_recv.at[t, g], pair)

    def middle(t, g):
        return remote(joint.at[t, g], from_inner.at[t, g], j_send.at[t], j_recv.at[t, g], across)

    def spread(t, g):
        piece = fin.at[c, t, g]
        return remote(piece, piece, s_send.at[t], s_recv.at[t, g], pair)

    def last(t, k, h):
        piece = fin.at[h, t, pl.ds(*shares[t][k])]
        return remote(piece, piece, h_send.at[t], h_recv.at[t, k], sib)

    def spread_skew(h):
        piece = fin.at[h, 1, slabs - 1]
        return remote(piece, piece, x_send.at[0], x_recv.at[0], skew)

    final = (1, len(shares[1]) - 1)

    def share_of(t, g):
        for k, (g0, size) in enumerate(shares[t]):
            if g == g0 + size - 1:
                return k
        return None

    def combine(t, q):
        g0, count = pieces[t][q]
        landed = ret.at[t, pl.ds(g0, count), pl.ds(1, n - 1)]
        remote(landed, landed, r_send.at[t], r_recv.at[t, q], sib).wait_recv()
        flat = jnp.concatenate([ret[t, g].reshape(rows, 128) for g in range(g0, g0 + count)], axis=1)
        if t == 0:
            flat = (flat.astype(F32) * slot_weight).astype(BF16)
        v = mm(back, flat).astype(BF16)
        for i in range(count):
            part[t, g0 + i] = v[:, i * 128 : (i + 1) * 128]

        @pl.when(outer)
        def _():
            for i in range(count):
                outward(t, g0 + i).start()

    def join(t, g):
        @pl.when(inner)
        def _():
            outward(t, g).wait_recv()
            joint[t, g] = (part[t, g].astype(F32) + from_outer[t, g].astype(F32)).astype(BF16)
            middle(t, g).start()

    def settle(t, g):
        k = share_of(t, g)

        @pl.when(inner)
        def _():
            middle(t, g).wait_recv()
            v = joint[t, g].astype(F32) + from_inner[t, g].astype(F32)
            fin[c, t, g] = v.astype(BF16)
            spread(t, g).start()
            if (t, k) == final:
                spread_skew(c).start()
            if k is not None:
                last(t, k, c).start()

    def arrive(t, g):
        k = share_of(t, g)

        @pl.when(outer)
        def _():
            spread(t, g).wait_recv()
            if k is not None and (t, k) != final:
                last(t, k, c).start()

    def place(t, k):
        if (t, k) == final:

            @pl.when(outer)
            def _():
                spread_skew(1 - c).wait_recv()

            @pl.when(inner)
            def _():
                last(t, k, 1 - c).wait_recv()
        else:
            last(t, k, 1 - c).wait_recv()
        g0, count = shares[t][k]
        for h in range(2):
            for g in range(g0, g0 + count):
                at = h * half + g * 128
                (output, input_grad)[t][:, at : at + 128] = fin[h, t, g]

    def turn(k):
        h, i = k // 3, k % 3
        step = half // 3
        x = slots[h, 0].reshape(rows, half)[:, i * step : (i + 1) * step]
        x_turned[h * half + i * step : h * half + (i + 1) * step] = x.T
        if i == 0:
            dy_rows[:, h * half : (h + 1) * half] = slots[h, 1].reshape(rows, half)
        if k == 5:
            hid_turned[...] = hid[...].T

    def gather():
        for j in range(parts):
            collect(1, j)

    def gathered():
        for j in range(parts):
            collected(1, j)

    plan = []

    def at(when, what, *args):
        plan.append((when, len(plan), what, args))

    def project(t, send_at, keep_at, done_at):
        for k in range(len(spans[t])):
            at(send_at[k], theirs, t, k)
            at(keep_at[k], ours, t, k)
            at(done_at[k], finish, t, k)

    beat = 0.7
    lag = 2.8
    project(0, (0.0, 0.9, 1.9), (0.45, 1.45, 2.4), (1.4, 2.35, 4.5))
    at(2.85, gather)
    at(3.6, down_own)
    at(4.55, gathered)
    for j in range(units // tile):
        at(4.6 + 0.9 * j, down_rest, j)
    project(1, (6.4, 8.3, 10.35), (7.6, 9.0, 11.1), (8.31, 10.34, 12.4))
    for k in range(6):
        at(12.8 + k, turn, k)
    free = [0.0] * 4
    ready = [1.4, 9.2]
    for t in range(2):
        for q, (g0, size) in enumerate(pieces[t]):
            free[0] = max(free[0], ready[t]) + beat * size
            landed = free[0] + lag + 0.5
            at(4.52 if t == 0 and q == 0 else landed, combine, t, q)
            for g in range(g0, g0 + size):
                when = landed
                for i, act in enumerate((join, settle, arrive)):
                    free[i + 1] = max(free[i + 1], when) + beat
                    when = free[i + 1] + lag
                    at(when + (1.5 if act is arrive else 0.0), act, t, g)
                k = share_of(t, g)
                if k is not None:
                    at(when + 2.8, place, t, k)
    for _, _, what, args in sorted(plan, key=lambda e: e[:2]):
        with jax.named_scope(what.__name__ + "".join(str(a) for a in args)):
            what(*args)

    with jax.named_scope("drain"):
        for t in range(2):
            sent = snd.at[t, far, held]
            remote(sent, sent, a_send.at[t, 0], a_recv.at[t, 0, 0], sib).wait_send()
            sent = snd.at[t, pl.ds(near[0], len(near))]
            remote(sent, sent, a_send.at[t, 1], a_recv.at[t, 0, 1], sib).wait_send()
            sent = slots.at[c, t, far, held]
            remote(sent, sent, d_send.at[t], d_recv.at[t, 0], pair).wait_send()
            sent = slots.at[c, t, pl.ds(1, n - 1)]
            remote(sent, sent, f_send.at[t], f_recv.at[t, 0], sib).wait_send()
            remote(core_snd.at[t], core_rcv.at[t], c_send.at[t], c_recv.at[t, 0], sib).wait_send()
            sent = ret_snd.at[t, :, pl.ds(1, n - 1)]
            remote(sent, sent, r_send.at[t], r_recv.at[t, 0], sib).wait_send()
            full = fin.at[c, t]
            short = fin.at[c, t, pl.ds(0, slabs - 1)] if t else full

            @pl.when(outer)
            def _():
                remote(short, short, h_send.at[t], h_recv.at[t, 0], sib).wait_send()
                sent = part.at[t]
                remote(sent, sent, s_send.at[t], s_recv.at[t, 0], pair).wait_send()

            @pl.when(inner)
            def _():
                remote(full, full, h_send.at[t], h_recv.at[t, 0], sib).wait_send()
                if t:
                    spread_skew(c).wait_send()
                sent = joint.at[t]
                remote(sent, sent, j_send.at[t], j_recv.at[t, 0], across).wait_send()
                sent = fin.at[c, t]
                remote(sent, sent, s_send.at[t], s_recv.at[t, 0], pair).wait_send()


def grads_kernel(
    step, output, input_grad, x_turned, dy_rows, hid_turned, hid_dy,
    output_hbm, input_grad_hbm, gate_hbm, up_hbm, down_hbm,
    gate, up, down, sem, g_sem,
):
    copies = [
        pltpu.make_async_copy(output, output_hbm, sem.at[0]),
        pltpu.make_async_copy(input_grad, input_grad_hbm, sem.at[1]),
    ]
    for cp in copies:
        cp.start()
    features = x_turned.shape[0]
    units = hid_turned.shape[0]

    def emit(k, at, value, buf, dst):
        buf[pl.ds(at, value.shape[0])] = value.astype(BF16)
        cp = pltpu.make_async_copy(
            buf.at[pl.ds(at, value.shape[0])], dst.at[pl.ds(at, value.shape[0])], g_sem.at[k]
        )
        cp.start()
        copies.append(cp)

    k = 0
    for at in range(0, features, step):
        x = x_turned[at : at + step]
        emit(k, at, mm(x, hid_dy[0]), gate, gate_hbm)
        emit(k + 1, at, mm(x, hid_dy[1]), up, up_hbm)
        k += 2
    rows_at = min(256, units)
    for at in range(0, units, rows_at):
        emit(k, at, mm(hid_turned[at : at + rows_at], dy_rows[...]), down, down_hbm)
        k += 1
    for cp in copies:
        cp.wait()


def fused(tokens, cotangent, routes, router_weight, w_gate, w_up, w_down):
    n = lax.axis_size("dp")
    toks, features = tokens.shape
    cap = capacity_of(toks, n)
    rows = n * cap
    half = features // 2
    units = w_gate.shape[2]
    tile = 512
    parts = 2
    slabs = half // 128
    third = slabs // 3
    even = [(g, 2) for g in range(0, slabs, 2)]
    pieces = ([(0, 1), (1, 1)] + even[1:], even[:-1] + [(slabs - 2, 1), (slabs - 1, 1)])
    most = max(len(p) for p in pieces)
    spans = (
        [(k * third, third) for k in range(3)],
        [(k * third, third) for k in range(3)],
    )
    shares = (
        [(k * third, third) for k in range(3)],
        [(0, third), (third, third), (2 * third, third - 2), (slabs - 2, 1), (slabs - 1, 1)],
    )
    vmem = pl.BlockSpec(memory_space=pltpu.VMEM)
    hbm = pl.BlockSpec(memory_space=pl.ANY)
    dma = pltpu.SemaphoreType.DMA
    V = pltpu.VMEM
    held = pl.pallas_call(
        functools.partial(routed_kernel, n, cap, tile, spans, pieces, shares),
        out_shape=(
            V((toks, features), BF16),
            V((toks, features), BF16),
            V((features, rows), BF16),
            V((rows, features), BF16),
            V((units, rows), BF16),
            V((2, rows, units), BF16),
        ),
        in_specs=[hbm] * 7,
        out_specs=(vmem,) * 6,
        scratch_shapes=[
            V((toks, features), BF16),
            V((toks, features), BF16),
            V((2, toks), jnp.int32),
            V((2, toks), F32),
            V((features, units), BF16),
            V((features, units), BF16),
            V((units, features), BF16),
            V((2, 2, n, cap, half), BF16),
            V((2, n, cap, half), BF16),
            V((rows, units), F32),
            V((rows, units), F32),
            V((rows, units), F32),
            V((rows, units), BF16),
            V((2, rows, half), BF16),
            V((2, rows, half), BF16),
            V((2, rows, half), F32),
            V((2, slabs, n, cap, 128), BF16),
            V((2, slabs, n, cap, 128), BF16),
            V((2, slabs, toks, 128), BF16),
            V((2, slabs, toks, 128), BF16),
            V((2, slabs, toks, 128), BF16),
            V((2, slabs, toks, 128), BF16),
            V((2, 2, slabs, toks, 128), BF16),
            dma((7,)),
            dma((2, 2)), dma((2, parts, n - 1)), dma((2,)), dma((2, parts)),
            dma((2,)), dma((2, parts)),
            dma((2,)), dma((2, 3)),
            dma((2,)), dma((2, most)),
            dma((2,)), dma((2, slabs)), dma((2,)), dma((2, slabs)), dma((2,)), dma((2, 5)),
            dma((1,)), dma((1,)),
        ],
        compiler_params=pltpu.CompilerParams(
            collective_id=0, has_side_effects=True, vmem_limit_bytes=54 * 1000 * 1000
        ),
        name="routed",
    )(tokens, cotangent, routes.T, router_weight.T, w_gate[0], w_up[0], w_down[0])

    step = 512
    output, input_grad, grad_gate, grad_up, grad_down = pl.pallas_call(
        functools.partial(grads_kernel, step),
        out_shape=(
            jax.ShapeDtypeStruct((toks, features), BF16),
            jax.ShapeDtypeStruct((toks, features), BF16),
            jax.ShapeDtypeStruct((features, units), BF16),
            jax.ShapeDtypeStruct((features, units), BF16),
            jax.ShapeDtypeStruct((units, features), BF16),
        ),
        in_specs=[vmem] * 6,
        out_specs=(hbm,) * 5,
        scratch_shapes=[
            V((features, units), BF16),
            V((features, units), BF16),
            V((units, features), BF16),
            dma((2,)),
            dma((2 * features // step + units // min(256, units),)),
        ],
        compiler_params=pltpu.CompilerParams(vmem_limit_bytes=50 * 1000 * 1000),
        name="grads",
    )(*held)
    return output, input_grad, grad_gate[None], grad_up[None], grad_down[None]


def slot_tables(routes, router_weight, experts, capacity):
    expert_ids = jnp.arange(experts, dtype=jnp.int32)
    hit_table = (routes[:, :, None] == expert_ids).astype(jnp.int32)
    per_token = jnp.sum(hit_table, axis=1)
    before = jnp.cumsum(per_token, axis=0) - per_token
    slot_of = jnp.sum(hit_table * before[:, None, :], axis=2)
    slot_ids = jnp.arange(capacity, dtype=jnp.int32)
    placed = hit_table[:, :, :, None] * (slot_of[:, :, None, None] == slot_ids).astype(jnp.int32)
    tok_rows = routes.shape[0]
    flat = placed.reshape(tok_rows, 2, experts * capacity).astype(jnp.float32)
    slot_weight = jnp.sum(flat * router_weight[:, :, None], axis=(0, 1))
    return (flat[:, 0], flat[:, 1], slot_weight)


def on_device(tokens, cotangent, routes, router_weight, w_gate, w_up, w_down):
    experts = lax.axis_size("dp")
    tok_rows, features = tokens.shape
    capacity = max(tok_rows * 3 // 8, tok_rows * 2 // experts, 2)
    local_rows = experts * capacity
    lead = (((0,), (0,)), ((), ()))
    trail = (((1,), (1,)), ((), ()))
    first_pick, second_pick, slot_weight = slot_tables(routes, router_weight, experts, capacity)
    picked = (first_pick + second_pick).astype(jnp.bfloat16)
    send_x = lax.dot_general(picked, tokens, lead, preferred_element_type=jnp.float32).astype(
        jnp.bfloat16
    )
    chosen_dy = lax.dot_general(picked, cotangent, lead, preferred_element_type=jnp.float32)
    send_dy = (chosen_dy * slot_weight[:, None]).astype(jnp.bfloat16)
    arrived_x, arrived_dy = (
        lax.all_to_all(
            send_x.reshape(experts, capacity, features),
            "dp",
            split_axis=0,
            concat_axis=0,
            tiled=True,
        ),
        lax.all_to_all(
            send_dy.reshape(experts, capacity, features),
            "dp",
            split_axis=0,
            concat_axis=0,
            tiled=True,
        ),
    )
    slot_x = arrived_x.reshape(local_rows, features)
    slot_dy = arrived_dy.reshape(local_rows, features)
    gate_w = w_gate[0]
    up_w = w_up[0]
    down_w = w_down[0]
    gate_pre = jnp.dot(slot_x, gate_w, preferred_element_type=jnp.float32)
    up_pre = jnp.dot(slot_x, up_w, preferred_element_type=jnp.float32)
    sigma = jax.nn.sigmoid(gate_pre)
    active = gate_pre * sigma
    hidden = (active * up_pre).astype(jnp.bfloat16)
    out_terms = jnp.dot(hidden, down_w, preferred_element_type=jnp.float32)
    hidden_dy = lax.dot_general(slot_dy, down_w, trail, preferred_element_type=jnp.float32)
    gate_dy = (hidden_dy * up_pre * sigma * (1.0 + gate_pre * (1.0 - sigma))).astype(jnp.bfloat16)
    up_dy = (hidden_dy * active).astype(jnp.bfloat16)
    grad_down = lax.dot_general(hidden, slot_dy, lead, preferred_element_type=jnp.float32).astype(
        jnp.bfloat16
    )
    grad_gate = lax.dot_general(slot_x, gate_dy, lead, preferred_element_type=jnp.float32).astype(
        jnp.bfloat16
    )
    grad_up = lax.dot_general(slot_x, up_dy, lead, preferred_element_type=jnp.float32).astype(
        jnp.bfloat16
    )
    back_terms = lax.dot_general(
        gate_dy, gate_w, trail, preferred_element_type=jnp.float32
    ) + lax.dot_general(up_dy, up_w, trail, preferred_element_type=jnp.float32)
    out_part, back_part = (
        lax.psum_scatter(
            out_terms.reshape(experts, capacity, features).astype(jnp.bfloat16),
            "fsdp",
            scatter_dimension=2,
            tiled=True,
        ).astype(jnp.float32),
        lax.psum_scatter(
            back_terms.reshape(experts, capacity, features).astype(jnp.bfloat16),
            "fsdp",
            scatter_dimension=2,
            tiled=True,
        ).astype(jnp.float32),
    )
    returned_out, returned_dx = (
        lax.all_to_all(
            out_part.astype(jnp.bfloat16), "dp", split_axis=0, concat_axis=0, tiled=True
        ),
        lax.all_to_all(
            back_part.astype(jnp.bfloat16), "dp", split_axis=0, concat_axis=0, tiled=True
        ),
    )
    width = out_part.shape[2]
    flat_out = returned_out.reshape(local_rows, width)
    flat_dx = returned_dx.reshape(local_rows, width)
    first_rows = jnp.dot(
        first_pick.astype(jnp.bfloat16), flat_out, preferred_element_type=jnp.float32
    )
    second_rows = jnp.dot(
        second_pick.astype(jnp.bfloat16), flat_out, preferred_element_type=jnp.float32
    )
    output = (router_weight[:, 0:1] * first_rows + router_weight[:, 1:2] * second_rows).astype(
        jnp.bfloat16
    )
    input_grad = jnp.dot(picked, flat_dx, preferred_element_type=jnp.float32).astype(jnp.bfloat16)
    output, input_grad = (
        lax.all_gather(output, "fsdp", axis=1, tiled=True),
        lax.all_gather(input_grad, "fsdp", axis=1, tiled=True),
    )
    return (output, input_grad, grad_gate[None], grad_up[None], grad_down[None])


def capacity_of(toks, experts):
    return max(toks * 3 // 8, toks * 2 // experts, 2)


def fits(mesh, toks, features, units):
    n, m = mesh.shape["dp"], mesh.shape["fsdp"]
    cap = capacity_of(toks, n)
    lines = n == 4 and m == 8
    whole = features % 1536 == 0 and units % 512 == 0 and cap % 32 == 0 and toks % 128 == 0
    rows = n * cap
    held = 6 * features * units + 2 * rows * (15 * features + 8 * units) + 20 * toks * features
    return lines and whole and held < 56 * 1000 * 1000


def solution(mesh):
    def step(tokens, cotangent, routes, router_weight, w_gate, w_up, w_down):
        body = fused if fits(mesh, *tokens.shape, w_gate.shape[2]) else on_device
        return body(tokens, cotangent, routes, router_weight, w_gate, w_up, w_down)

    return jax.shard_map(
        step,
        mesh=mesh,
        in_specs=(
            P("dp", None),
            P("dp", None),
            P("dp", None),
            P("dp", None),
            P("dp", None, "fsdp"),
            P("dp", None, "fsdp"),
            P("dp", "fsdp", None),
        ),
        out_specs=(
            P("dp", None),
            P("dp", None),
            P("dp", None, "fsdp"),
            P("dp", None, "fsdp"),
            P("dp", "fsdp", None),
        ),
        check_vma=False,
    )
```

```python
import functools

import jax
import jax.numpy as jnp
from jax import lax
from jax.experimental import pallas as pl
from jax.experimental.pallas import tpu as pltpu
from jax.sharding import PartitionSpec as P

MESH = pl.DeviceIdType.MESH
BF16 = jnp.bfloat16
F32 = jnp.float32
LEAD = (((0,), (0,)), ((), ()))
TRAIL = (((1,), (1,)), ((), ()))


def flip(a, mask):
    bit = 1
    while bit <= mask:
        if mask & bit:
            a = a + bit - 2 * bit * ((a // bit) % 2)
        bit *= 2
    return a


def xor(v, a, n):
    out = v - v
    bit = 1
    while bit < n:
        x, y = (v // bit) % 2, (a // bit) % 2
        out = out + bit * (x + y - 2 * x * y)
        bit *= 2
    return out


def mm(a, b, dims=(((1,), (0,)), ((), ()))):
    return lax.dot_general(a, b, dims, preferred_element_type=F32)


def routed_kernel(
    n, cap, tile, spans, pieces, shares,
    tokens_hbm, cotangent_hbm, routes_hbm, rweight_hbm, wg_hbm, wu_hbm, wd_hbm,
    output, input_grad, x_turned, dy_rows, hid_turned, hid_dy,
    tok, cot, rts, rwt, wg, wu, wd, slots, snd, gpre, upre, hacc, hid,
    core_snd, core_rcv, own, ret_snd, ret, part, from_outer, joint, from_inner, fin,
    w_sem, a_send, a_recv, d_send, d_recv, f_send, f_recv, c_send, c_recv, r_send, r_recv,
    s_send, s_recv, j_send, j_recv, h_send, h_recv, x_send, x_recv,
):
    d = lax.axis_index("dp")
    f = lax.axis_index("fsdp")
    c = f % 2
    z = f // 2
    sib = (d, flip(f, 1))
    pair = (d, flip(f, 2))
    across = (d, 2 * (3 - z) + c)
    skew = (d, flip(f, 3))
    outer = (z % 3) == 0
    inner = (z % 3) != 0
    toks, features = tok.shape
    half = features // 2
    rows = n * cap
    units = gpre.shape[1]
    slabs = half // 128
    order = sorted(range(1, n), key=lambda m: -bin(m).count("1"))
    far = order[0]
    near = order[1:]
    share = cap // 2

    def remote(src, dst, ssem, rsem, dev):
        return pltpu.make_async_remote_copy(
            src_ref=src, dst_ref=dst, send_sem=ssem, recv_sem=rsem,
            device_id=dev, device_id_type=MESH,
        )

    barrier = pltpu.get_barrier_semaphore()
    friends = [(flip(d, m), f) for m in order] + [sib, pair, across, skew]
    for dev in friends:
        pl.semaphore_signal(barrier, inc=1, device_id=dev, device_id_type=MESH)

    loads = [
        pltpu.make_async_copy(s, t, w_sem.at[k])
        for k, (s, t) in enumerate(
            (
                (routes_hbm, rts), (rweight_hbm, rwt), (tokens_hbm, tok), (cotangent_hbm, cot),
                (wg_hbm, wg), (wu_hbm, wu), (wd_hbm, wd),
            )
        )
    ]
    for load in loads:
        load.start()
    with jax.named_scope('w_small'):
        loads[0].wait()
        loads[1].wait()

    slot_row = lax.broadcasted_iota(jnp.int32, (rows, toks), 0)
    m_of = slot_row // cap
    e_of = xor(m_of, d, n)
    s_of = (slot_row % cap).astype(F32)
    r = rts[...]
    hit0 = r[0:1, :] == e_of
    hit1 = r[1:2, :] == e_of
    per_token = jnp.where(hit0 | hit1, 1.0, 0.0).astype(BF16)
    earlier = (
        lax.broadcasted_iota(jnp.int32, (toks, toks), 0)
        < lax.broadcasted_iota(jnp.int32, (toks, toks), 1)
    )
    before = mm(per_token, jnp.where(earlier, 1.0, 0.0).astype(BF16))
    here = before == s_of
    first = jnp.where(hit0 & here, 1.0, 0.0)
    second = jnp.where(hit1 & here, 1.0, 0.0)
    rw = rwt[...]
    slot_weight = jnp.sum(first * rw[0:1, :] + second * rw[1:2, :], axis=1, keepdims=True)
    picked = (first + second).astype(BF16)
    same = (
        lax.broadcasted_iota(jnp.int32, (toks, toks), 0)
        == lax.broadcasted_iota(jnp.int32, (toks, toks), 1)
    )
    back = mm(jnp.where(same, 1.0, 0.0).astype(BF16), picked, TRAIL).astype(BF16)

    mine = pl.ds(pl.multiple_of(c * half, 128), half)
    other = pl.ds(pl.multiple_of((1 - c) * half, 128), half)

    def build(t):
        src = (tok, cot)[t]
        v = mm(picked, src[:, mine])
        u = mm(picked[:cap], src[:, other])
        if t:
            v = v * slot_weight
            u = u * slot_weight[:cap]
        snd[t] = v.astype(BF16).reshape(n, cap, half)
        slots[c, t, 0] = v[:cap].astype(BF16)
        slots[1 - c, t, 0] = u.astype(BF16)

    held = pl.ds(pl.multiple_of((z % 2) * share, 16), share)
    missing = pl.ds(pl.multiple_of((1 - z % 2) * share, 16), share)
    parts = a_recv.shape[1]
    depth = half // parts

    def part_of(j):
        return pl.ds(j * depth, depth)

    def direct(t, m, j):
        dev = (flip(d, m), f)
        if m == far:
            return remote(
                snd.at[t, m, held, part_of(j)], slots.at[c, t, m, held, part_of(j)],
                a_send.at[t, 0], a_recv.at[t, j, 0], dev,
            )
        return remote(
            snd.at[t, m, :, part_of(j)], slots.at[c, t, m, :, part_of(j)],
            a_send.at[t, 1], a_recv.at[t, j, m], dev,
        )

    def dispatch(t):
        for j in range(parts):
            direct(t, far, j).start()
        for j in range(parts):
            for m in near:
                direct(t, m, j).start()

    def relay(t, j, rows_at):
        piece = slots.at[c, t, far, rows_at, part_of(j)]
        return remote(piece, piece, d_send.at[t], d_recv.at[t, j], pair)

    def forward(t, j, k):
        if k == 0:
            piece = slots.at[c, t, far, held, part_of(j)]
        elif k == n:
            piece = slots.at[c, t, far, missing, part_of(j)]
        else:
            piece = slots.at[c, t, k, :, part_of(j)]
        return remote(piece, piece, f_send.at[t], f_recv.at[t, j], sib)

    def relay_far(t, j):
        direct(t, far, j).wait_recv()
        relay(t, j, held).start()
        forward(t, j, 0).start()

    def collect(t, j):
        for m in near:
            direct(t, m, j).wait_recv()
            forward(t, j, m).start()
        relay(t, j, missing).wait_recv()
        forward(t, j, n).start()

    def collected(t, j):
        theirs = slots.at[1 - c, t, pl.ds(1, n - 1), :, part_of(j)]
        remote(theirs, theirs, f_send.at[t], f_recv.at[t, j], sib).wait_recv()

    loads[2].wait()
    with jax.named_scope("build0"):
        build(0)
    with jax.named_scope("w_barrier"):
        pl.semaphore_wait(barrier, len(friends))
    dispatch(0)
    loads[3].wait()
    with jax.named_scope("build1"):
        build(1)
    dispatch(1)

    def at_half(h):
        return pl.ds(pl.multiple_of(h * half, 128), half)

    def activate(at, cols, g, u):
        gpre[at, cols] = g
        upre[at, cols] = u
        hid[at, cols] = (g * jax.nn.sigmoid(g) * u).astype(BF16)

    def gate_up(m0, blocks, h, k, first=False, final=False):
        at = pl.ds(m0 * cap, blocks * cap)
        depth_at = pl.ds(pl.multiple_of(h * half + k * depth, 128), depth)
        for j in range(units // tile):
            cols = pl.ds(j * tile, tile)
            x = slots[h, 0, m0 : m0 + blocks, :, part_of(k)].reshape(blocks * cap, depth)
            g = mm(x, wg[depth_at, cols])
            u = mm(x, wu[depth_at, cols])
            if not first:
                g = g + gpre[at, cols]
                u = u + upre[at, cols]
            gpre[at, cols] = g
            upre[at, cols] = u
            if final:
                hid[at, cols] = (g * jax.nn.sigmoid(g) * u).astype(BF16)

    def scoped(what, *args, **kw):
        with jax.named_scope(what.__name__ + "".join(str(a) for a in args if isinstance(a, int))):
            what(*args, **kw)

    loads[4].wait()
    loads[5].wait()
    for i in range(2 * parts):
        scoped(
            gate_up, 0, 1, c if i < parts else 1 - c, i % parts,
            first=i == 0, final=i == 2 * parts - 1,
        )
    for j in range(parts):
        scoped(relay_far, 0, j)
    others = n - 1
    for j in range(parts):
        scoped(collect, 0, j)
        scoped(gate_up, 1, others, c, j, first=j == 0)
        if 0 < j < parts - 1:
            scoped(collected, 0, j - 1)
            scoped(gate_up, 1, others, 1 - c, j - 1)
    for j in range(max(0, parts - 2), parts):
        scoped(collected, 0, j)
        scoped(gate_up, 1, others, 1 - c, j, final=j == parts - 1)
        if j < parts - 1:
            for k in range(parts - 1):
                scoped(relay_far, 1, k)
    scoped(relay_far, 1, parts - 1)
    loads[6].wait()

    def span(t, k):
        return pl.ds(spans[t][k][0] * 128, spans[t][k][1] * 128)

    def swap(t, k):
        at = span(t, k)
        return remote(
            core_snd.at[t, :, at], core_rcv.at[t, :, at], c_send.at[t], c_recv.at[t, k], sib
        )

    def returned(t, q, m):
        at = pl.ds(*pieces[t][q])
        return remote(
            ret_snd.at[t, at, m], ret.at[t, at, m], r_send.at[t], r_recv.at[t, q], (flip(d, m), f)
        )

    def term(t, cols):
        if t == 0:
            return mm(hid[...], wd[:, cols])
        return mm(hid_dy[0], wg[cols, :], TRAIL) + mm(hid_dy[1], wu[cols, :], TRAIL)

    def theirs(t, k):
        g0, size = spans[t][k]
        at = pl.multiple_of((1 - c) * half + g0 * 128, 128)
        core_snd[t, :, span(t, k)] = term(t, pl.ds(at, size * 128)).astype(BF16)
        swap(t, k).start()

    def ours(t, k):
        g0, size = spans[t][k]
        at = pl.multiple_of(c * half + g0 * 128, 128)
        own[t, :, span(t, k)] = term(t, pl.ds(at, size * 128))

    def finish(t, k):
        swap(t, k).wait_recv()
        low, size = spans[t][k]
        for q, (g0, count) in enumerate(pieces[t]):
            if not low <= g0 < low + size:
                continue
            for m in order + [0]:
                for g in range(g0, g0 + count):
                    cols = pl.ds(g * 128, 128)
                    at = pl.ds(m * cap, cap)
                    v = own[t, at, cols] + core_rcv[t, at, cols].astype(F32)
                    (ret_snd if m else ret)[t, g, m] = v.astype(BF16)
                if m:
                    returned(t, q, m).start()

    def down_own():
        for j in range(units // tile):
            cols = pl.ds(j * tile, tile)
            hacc[:, cols] = mm(slots[c, 1].reshape(rows, half), wd[cols, mine], TRAIL)

    def down_rest(j):
        cols = pl.ds(j * tile, tile)
        hdy = hacc[:, cols] + mm(slots[1 - c, 1].reshape(rows, half), wd[cols, other], TRAIL)
        g = gpre[:, cols]
        sig = jax.nn.sigmoid(g)
        hid_dy[0, :, cols] = (hdy * upre[:, cols] * sig * (1.0 + g * (1.0 - sig))).astype(BF16)
        hid_dy[1, :, cols] = (hdy * (g * sig)).astype(BF16)

    def outward(t, g):
        return remote(part.at[t, g], from_outer.at[t, g], s_send.at[t], s_recv.at[t, g], pair)

    def middle(t, g):
        return remote(joint.at[t, g], from_inner.at[t, g], j_send.at[t], j_recv.at[t, g], across)

    def spread(t, g):
        piece = fin.at[c, t, g]
        return remote(piece, piece, s_send.at[t], s_recv.at[t, g], pair)

    def last(t, k, h):
        piece = fin.at[h, t, pl.ds(*shares[t][k])]
        return remote(piece, piece, h_send.at[t], h_recv.at[t + k], sib)

    def spread_skew(h):
        piece = fin.at[h, 1, slabs - 1]
        return remote(piece, piece, x_send.at[0], x_recv.at[0], skew)

    final = (1, len(shares[1]) - 1)

    def share_of(t, g):
        for k, (g0, size) in enumerate(shares[t]):
            if g == g0 + size - 1:
                return k
        return None

    def combine(t, q):
        g0, count = pieces[t][q]
        landed = ret.at[t, pl.ds(g0, count), pl.ds(1, n - 1)]
        remote(landed, landed, r_send.at[t], r_recv.at[t, q], sib).wait_recv()
        flat = jnp.concatenate([ret[t, g].reshape(rows, 128) for g in range(g0, g0 + count)], axis=1)
        if t == 0:
            flat = (flat.astype(F32) * slot_weight).astype(BF16)
        v = mm(back, flat).astype(BF16)
        for i in range(count):
            part[t, g0 + i] = v[:, i * 128 : (i + 1) * 128]

        @pl.when(outer)
        def _():
            for i in range(count):
                outward(t, g0 + i).start()

    def join(t, g):
        @pl.when(inner)
        def _():
            outward(t, g).wait_recv()
            joint[t, g] = (part[t, g].astype(F32) + from_outer[t, g].astype(F32)).astype(BF16)
            middle(t, g).start()

    def settle(t, g):
        k = share_of(t, g)

        @pl.when(inner)
        def _():
            middle(t, g).wait_recv()
            v = joint[t, g].astype(F32) + from_inner[t, g].astype(F32)
            fin[c, t, g] = v.astype(BF16)
            spread(t, g).start()
            if (t, k) == final:
                spread_skew(c).start()
            if k is not None:
                last(t, k, c).start()

    def arrive(t, g):
        k = share_of(t, g)

        @pl.when(outer)
        def _():
            spread(t, g).wait_recv()
            if k is not None and (t, k) != final:
                last(t, k, c).start()

    def place(t, k):
        if (t, k) == final:

            @pl.when(outer)
            def _():
                spread_skew(1 - c).wait_recv()

            @pl.when(inner)
            def _():
                last(t, k, 1 - c).wait_recv()
        else:
            last(t, k, 1 - c).wait_recv()
        g0, count = shares[t][k]
        for h in range(2):
            for g in range(g0, g0 + count):
                at = h * half + g * 128
                (output, input_grad)[t][:, at : at + 128] = fin[h, t, g]

    def turn(k):
        h, i = k // 3, k % 3
        step = half // 3
        x = slots[h, 0].reshape(rows, half)[:, i * step : (i + 1) * step]
        x_turned[h * half + i * step : h * half + (i + 1) * step] = x.T
        if i == 0:
            dy_rows[:, h * half : (h + 1) * half] = slots[h, 1].reshape(rows, half)
        if k == 5:
            hid_turned[...] = hid[...].T

    def gather():
        for j in range(parts):
            collect(1, j)

    def gathered():
        for j in range(parts):
            collected(1, j)

    plan = []

    def at(when, what, *args):
        plan.append((when, len(plan), what, args))

    def project(t, send_at, keep_at, done_at):
        for k in range(len(spans[t])):
            at(send_at[k], theirs, t, k)
            at(keep_at[k], ours, t, k)
            at(done_at[k], finish, t, k)

    beat = 0.7
    lag = 2.8
    project(0, (0.0, 0.9, 1.9), (0.45, 1.45, 2.4), (1.4, 2.35, 4.5))
    at(2.85, gather)
    at(3.6, down_own)
    at(4.55, gathered)
    for j in range(units // tile):
        at(4.6 + 0.9 * j, down_rest, j)
    project(1, (6.4, 8.3, 10.35), (7.6, 9.0, 11.1), (8.31, 10.34, 12.4))
    for k in range(6):
        at(12.8 + k, turn, k)
    free = [0.0] * 4
    ready = [1.4, 9.2]
    for t in range(2):
        for q, (g0, size) in enumerate(pieces[t]):
            free[0] = max(free[0], ready[t]) + beat * size
            landed = free[0] + lag + 0.5
            at(4.52 if t == 0 and q == 0 else landed, combine, t, q)
            for g in range(g0, g0 + size):
                when = landed
                for i, act in enumerate((join, settle, arrive)):
                    free[i + 1] = max(free[i + 1], when) + beat
                    when = free[i + 1] + lag
                    at(when + (1.5 if act is arrive else 0.0), act, t, g)
                k = share_of(t, g)
                if k is not None:
                    at(when + 2.8, place, t, k)
    for _, _, what, args in sorted(plan, key=lambda e: e[:2]):
        with jax.named_scope(what.__name__ + "".join(str(a) for a in args)):
            what(*args)

    with jax.named_scope("drain"):
        for t in range(2):
            sent = snd.at[t, far, held]
            remote(sent, sent, a_send.at[t, 0], a_recv.at[t, 0, 0], sib).wait_send()
            sent = snd.at[t, pl.ds(near[0], len(near))]
            remote(sent, sent, a_send.at[t, 1], a_recv.at[t, 0, 1], sib).wait_send()
            sent = slots.at[c, t, far, held]
            remote(sent, sent, d_send.at[t], d_recv.at[t, 0], pair).wait_send()
            sent = slots.at[c, t, pl.ds(1, n - 1)]
            remote(sent, sent, f_send.at[t], f_recv.at[t, 0], sib).wait_send()
            remote(core_snd.at[t], core_rcv.at[t], c_send.at[t], c_recv.at[t, 0], sib).wait_send()
            sent = ret_snd.at[t, :, pl.ds(1, n - 1)]
            remote(sent, sent, r_send.at[t], r_recv.at[t, 0], sib).wait_send()
            full = fin.at[c, t]
            short = fin.at[c, t, pl.ds(0, slabs - 1)] if t else full

            @pl.when(outer)
            def _():
                remote(short, short, h_send.at[t], h_recv.at[t], sib).wait_send()
                sent = part.at[t]
                remote(sent, sent, s_send.at[t], s_recv.at[t, 0], pair).wait_send()

            @pl.when(inner)
            def _():
                remote(full, full, h_send.at[t], h_recv.at[t], sib).wait_send()
                if t:
                    spread_skew(c).wait_send()
                sent = joint.at[t]
                remote(sent, sent, j_send.at[t], j_recv.at[t, 0], across).wait_send()
                sent = fin.at[c, t]
                remote(sent, sent, s_send.at[t], s_recv.at[t, 0], pair).wait_send()


def grads_kernel(
    step, output, input_grad, x_turned, dy_rows, hid_turned, hid_dy,
    output_hbm, input_grad_hbm, gate_hbm, up_hbm, down_hbm,
    gate, up, down, sem, g_sem,
):
    copies = [
        pltpu.make_async_copy(output, output_hbm, sem.at[0]),
        pltpu.make_async_copy(input_grad, input_grad_hbm, sem.at[1]),
    ]
    for cp in copies:
        cp.start()
    features = x_turned.shape[0]
    units = hid_turned.shape[0]

    def emit(k, at, value, buf, dst):
        buf[pl.ds(at, value.shape[0])] = value.astype(BF16)
        cp = pltpu.make_async_copy(
            buf.at[pl.ds(at, value.shape[0])], dst.at[pl.ds(at, value.shape[0])], g_sem.at[k]
        )
        cp.start()
        copies.append(cp)

    k = 0
    for at in range(0, features, step):
        x = x_turned[at : at + step]
        emit(k, at, mm(x, hid_dy[0]), gate, gate_hbm)
        emit(k + 1, at, mm(x, hid_dy[1]), up, up_hbm)
        k += 2
    rows_at = min(256, units)
    for at in range(0, units, rows_at):
        emit(k, at, mm(hid_turned[at : at + rows_at], dy_rows[...]), down, down_hbm)
        k += 1
    for cp in copies:
        cp.wait()


def fused(tokens, cotangent, routes, router_weight, w_gate, w_up, w_down):
    n = lax.axis_size("dp")
    toks, features = tokens.shape
    cap = capacity_of(toks, n)
    rows = n * cap
    half = features // 2
    units = w_gate.shape[2]
    tile = 512
    parts = 2
    slabs = half // 128
    third = slabs // 3
    even = [(g, 2) for g in range(0, slabs, 2)]
    pieces = ([(0, 1), (1, 1)] + even[1:], even[:-1] + [(slabs - 2, 1), (slabs - 1, 1)])
    most = max(len(p) for p in pieces)
    spans = (
        [(k * third, third) for k in range(3)],
        [(k * third, third) for k in range(3)],
    )
    shares = (
        [(0, slabs)],
        [(0, slabs - 4), (slabs - 4, 2), (slabs - 2, 1), (slabs - 1, 1)],
    )
    vmem = pl.BlockSpec(memory_space=pltpu.VMEM)
    hbm = pl.BlockSpec(memory_space=pl.ANY)
    dma = pltpu.SemaphoreType.DMA
    V = pltpu.VMEM
    held = pl.pallas_call(
        functools.partial(routed_kernel, n, cap, tile, spans, pieces, shares),
        out_shape=(
            V((toks, features), BF16),
            V((toks, features), BF16),
            V((features, rows), BF16),
            V((rows, features), BF16),
            V((units, rows), BF16),
            V((2, rows, units), BF16),
        ),
        in_specs=[hbm] * 7,
        out_specs=(vmem,) * 6,
        scratch_shapes=[
            V((toks, features), BF16),
            V((toks, features), BF16),
            V((2, toks), jnp.int32),
            V((2, toks), F32),
            V((features, units), BF16),
            V((features, units), BF16),
            V((units, features), BF16),
            V((2, 2, n, cap, half), BF16),
            V((2, n, cap, half), BF16),
            V((rows, units), F32),
            V((rows, units), F32),
            V((rows, units), F32),
            V((rows, units), BF16),
            V((2, rows, half), BF16),
            V((2, rows, half), BF16),
            V((2, rows, half), F32),
            V((2, slabs, n, cap, 128), BF16),
            V((2, slabs, n, cap, 128), BF16),
            V((2, slabs, toks, 128), BF16),
            V((2, slabs, toks, 128), BF16),
            V((2, slabs, toks, 128), BF16),
            V((2, slabs, toks, 128), BF16),
            V((2, 2, slabs, toks, 128), BF16),
            dma((7,)),
            dma((2, 2)), dma((2, parts, n - 1)), dma((2,)), dma((2, parts)),
            dma((2,)), dma((2, parts)),
            dma((2,)), dma((2, 3)),
            dma((2,)), dma((2, most)),
            dma((2,)), dma((2, slabs)), dma((2,)), dma((2, slabs)), dma((2,)), dma((5,)),
            dma((1,)), dma((1,)),
        ],
        compiler_params=pltpu.CompilerParams(
            collective_id=0, has_side_effects=True, vmem_limit_bytes=54 * 1000 * 1000
        ),
        name="routed",
    )(tokens, cotangent, routes.T, router_weight.T, w_gate[0], w_up[0], w_down[0])

    step = 512
    output, input_grad, grad_gate, grad_up, grad_down = pl.pallas_call(
        functools.partial(grads_kernel, step),
        out_shape=(
            jax.ShapeDtypeStruct((toks, features), BF16),
            jax.ShapeDtypeStruct((toks, features), BF16),
            jax.ShapeDtypeStruct((features, units), BF16),
            jax.ShapeDtypeStruct((features, units), BF16),
            jax.ShapeDtypeStruct((units, features), BF16),
        ),
        in_specs=[vmem] * 6,
        out_specs=(hbm,) * 5,
        scratch_shapes=[
            V((features, units), BF16),
            V((features, units), BF16),
            V((units, features), BF16),
            dma((2,)),
            dma((2 * features // step + units // min(256, units),)),
        ],
        compiler_params=pltpu.CompilerParams(vmem_limit_bytes=50 * 1000 * 1000),
        name="grads",
    )(*held)
    return output, input_grad, grad_gate[None], grad_up[None], grad_down[None]


def slot_tables(routes, router_weight, experts, capacity):
    expert_ids = jnp.arange(experts, dtype=jnp.int32)
    hit_table = (routes[:, :, None] == expert_ids).astype(jnp.int32)
    per_token = jnp.sum(hit_table, axis=1)
    before = jnp.cumsum(per_token, axis=0) - per_token
    slot_of = jnp.sum(hit_table * before[:, None, :], axis=2)
    slot_ids = jnp.arange(capacity, dtype=jnp.int32)
    placed = hit_table[:, :, :, None] * (slot_of[:, :, None, None] == slot_ids).astype(jnp.int32)
    tok_rows = routes.shape[0]
    flat = placed.reshape(tok_rows, 2, experts * capacity).astype(jnp.float32)
    slot_weight = jnp.sum(flat * router_weight[:, :, None], axis=(0, 1))
    return (flat[:, 0], flat[:, 1], slot_weight)


def on_device(tokens, cotangent, routes, router_weight, w_gate, w_up, w_down):
    experts = lax.axis_size("dp")
    tok_rows, features = tokens.shape
    capacity = max(tok_rows * 3 // 8, tok_rows * 2 // experts, 2)
    local_rows = experts * capacity
    lead = (((0,), (0,)), ((), ()))
    trail = (((1,), (1,)), ((), ()))
    first_pick, second_pick, slot_weight = slot_tables(routes, router_weight, experts, capacity)
    picked = (first_pick + second_pick).astype(jnp.bfloat16)
    send_x = lax.dot_general(picked, tokens, lead, preferred_element_type=jnp.float32).astype(
        jnp.bfloat16
    )
    chosen_dy = lax.dot_general(picked, cotangent, lead, preferred_element_type=jnp.float32)
    send_dy = (chosen_dy * slot_weight[:, None]).astype(jnp.bfloat16)
    arrived_x, arrived_dy = (
        lax.all_to_all(
            send_x.reshape(experts, capacity, features),
            "dp",
            split_axis=0,
            concat_axis=0,
            tiled=True,
        ),
        lax.all_to_all(
            send_dy.reshape(experts, capacity, features),
            "dp",
            split_axis=0,
            concat_axis=0,
            tiled=True,
        ),
    )
    slot_x = arrived_x.reshape(local_rows, features)
    slot_dy = arrived_dy.reshape(local_rows, features)
    gate_w = w_gate[0]
    up_w = w_up[0]
    down_w = w_down[0]
    gate_pre = jnp.dot(slot_x, gate_w, preferred_element_type=jnp.float32)
    up_pre = jnp.dot(slot_x, up_w, preferred_element_type=jnp.float32)
    sigma = jax.nn.sigmoid(gate_pre)
    active = gate_pre * sigma
    hidden = (active * up_pre).astype(jnp.bfloat16)
    out_terms = jnp.dot(hidden, down_w, preferred_element_type=jnp.float32)
    hidden_dy = lax.dot_general(slot_dy, down_w, trail, preferred_element_type=jnp.float32)
    gate_dy = (hidden_dy * up_pre * sigma * (1.0 + gate_pre * (1.0 - sigma))).astype(jnp.bfloat16)
    up_dy = (hidden_dy * active).astype(jnp.bfloat16)
    grad_down = lax.dot_general(hidden, slot_dy, lead, preferred_element_type=jnp.float32).astype(
        jnp.bfloat16
    )
    grad_gate = lax.dot_general(slot_x, gate_dy, lead, preferred_element_type=jnp.float32).astype(
        jnp.bfloat16
    )
    grad_up = lax.dot_general(slot_x, up_dy, lead, preferred_element_type=jnp.float32).astype(
        jnp.bfloat16
    )
    back_terms = lax.dot_general(
        gate_dy, gate_w, trail, preferred_element_type=jnp.float32
    ) + lax.dot_general(up_dy, up_w, trail, preferred_element_type=jnp.float32)
    out_part, back_part = (
        lax.psum_scatter(
            out_terms.reshape(experts, capacity, features).astype(jnp.bfloat16),
            "fsdp",
            scatter_dimension=2,
            tiled=True,
        ).astype(jnp.float32),
        lax.psum_scatter(
            back_terms.reshape(experts, capacity, features).astype(jnp.bfloat16),
            "fsdp",
            scatter_dimension=2,
            tiled=True,
        ).astype(jnp.float32),
    )
    returned_out, returned_dx = (
        lax.all_to_all(
            out_part.astype(jnp.bfloat16), "dp", split_axis=0, concat_axis=0, tiled=True
        ),
        lax.all_to_all(
            back_part.astype(jnp.bfloat16), "dp", split_axis=0, concat_axis=0, tiled=True
        ),
    )
    width = out_part.shape[2]
    flat_out = returned_out.reshape(local_rows, width)
    flat_dx = returned_dx.reshape(local_rows, width)
    first_rows = jnp.dot(
        first_pick.astype(jnp.bfloat16), flat_out, preferred_element_type=jnp.float32
    )
    second_rows = jnp.dot(
        second_pick.astype(jnp.bfloat16), flat_out, preferred_element_type=jnp.float32
    )
    output = (router_weight[:, 0:1] * first_rows + router_weight[:, 1:2] * second_rows).astype(
        jnp.bfloat16
    )
    input_grad = jnp.dot(picked, flat_dx, preferred_element_type=jnp.float32).astype(jnp.bfloat16)
    output, input_grad = (
        lax.all_gather(output, "fsdp", axis=1, tiled=True),
        lax.all_gather(input_grad, "fsdp", axis=1, tiled=True),
    )
    return (output, input_grad, grad_gate[None], grad_up[None], grad_down[None])


def capacity_of(toks, experts):
    return max(toks * 3 // 8, toks * 2 // experts, 2)


def fits(mesh, toks, features, units):
    n, m = mesh.shape["dp"], mesh.shape["fsdp"]
    cap = capacity_of(toks, n)
    lines = n == 4 and m == 8
    whole = features % 1536 == 0 and units % 512 == 0 and cap % 32 == 0 and toks % 128 == 0
    rows = n * cap
    held = 6 * features * units + 2 * rows * (15 * features + 8 * units) + 20 * toks * features
    return lines and whole and held < 56 * 1000 * 1000


def solution(mesh):
    def step(tokens, cotangent, routes, router_weight, w_gate, w_up, w_down):
        body = fused if fits(mesh, *tokens.shape, w_gate.shape[2]) else on_device
        return body(tokens, cotangent, routes, router_weight, w_gate, w_up, w_down)

    return jax.shard_map(
        step,
        mesh=mesh,
        in_specs=(
            P("dp", None),
            P("dp", None),
            P("dp", None),
            P("dp", None),
            P("dp", None, "fsdp"),
            P("dp", None, "fsdp"),
            P("dp", "fsdp", None),
        ),
        out_specs=(
            P("dp", None),
            P("dp", None),
            P("dp", None, "fsdp"),
            P("dp", None, "fsdp"),
            P("dp", "fsdp", None),
        ),
        check_vma=False,
    )
```
